128 devices in a mesh: rep: 16 (over z, x_lo, core), tp: 8 (over y, x_hi).
Axes of the slice: x: 4 (x_hi: 2, x_lo: 2; x = x_hi * 2 + x_lo), y: 4, z: 4, core: 2. Of those that a mesh axis runs over, the one named last changes fastest.
Arguments:
- hidden_state: bfloat16 [64, 3584], P('rep'), may hold values from -6 to 6
- lengths: int32 [64], P('rep'), may hold values from 1 to 4096, as said below
- old_qkv: bfloat16 [3584, 4608], P(None, 'tp'), may hold values from -0.09375 to 0.09375
- old_out: bfloat16 [3584, 3584], P(None, 'tp'), may hold values from -0.09375 to 0.09375
- cache_keys: bfloat16 [64, 4096, 512], P('rep', 'tp'), may hold values from -64 to 64
- cache_values: bfloat16 [64, 4096, 512], P('rep', 'tp'), may hold values from -6 to 6
- new_qkv: bfloat16 [3584, 4608], P(('rep', 'tp')), may hold values from -0.09375 to 0.09375
- new_out: bfloat16 [3584, 3584], P(('rep', 'tp')), may hold values from -0.09375 to 0.09375
Outputs:
- decoded: bfloat16 [64, 3584], P('rep', 'tp')
- resharded_qkv: bfloat16 [3584, 4608], P(None, 'tp')
- resharded_out: bfloat16 [3584, 3584], P(None, 'tp')
The draws below stay inside these ranges and needn't reach their ends.
Inputs may be any that keep to these rules, and one draw needn't show every extreme that they name: Every sequence has 1 to 4096 cached tokens, held in positions 0 to lengths - 1; in every draw some sequence fills its cache.
All inputs are finite; a program needn't handle non-finite values.
Results may differ from the reference program's by a relative error of at most 0.012.
Values may be sent and summed in bfloat16 or wider, within the bound.
A program may use at most 128 MiB of HBM per device.

```python
import jax
import jax.numpy as jnp
from jax import lax

D = 3584
HQ = 28
KVH = 4
HD = 128
SEQS = 64
CACHE_LEN = 4096
COLS = 4608


def draw_lengths(key, part):
    drawn = jax.random.randint(key, (SEQS,), 1, CACHE_LEN + 1)
    chosen = jax.random.randint(jax.random.fold_in(key, 7), (), 0, SEQS)
    return jnp.where(jnp.arange(SEQS) == chosen, CACHE_LEN, drawn).astype(jnp.int32)


def draw_cache_keys(key, part):
    drawn = jax.random.normal(key, (SEQS, CACHE_LEN, KVH * HD), jnp.float32)
    return jnp.clip(drawn, -64.0, 64.0).astype(jnp.bfloat16)


def levels(rng, dims, pieces, least, largest):
    level = 1.0
    for axis_at, shards_of in pieces:
        steps = jax.random.uniform(jax.random.fold_in(jax.random.fold_in(rng, 6), axis_at), (shards_of,), jnp.float32, least / len(pieces), largest / len(pieces))
        level = level * jnp.repeat(jnp.exp(steps), dims[axis_at] // shards_of).reshape((-1,) + (1,) * (len(dims) - 1 - axis_at))
    return level


def bell_draw(stream_key, shape, deviation, bound, cuts=(), kind=jnp.bfloat16):
    values = deviation * jax.random.normal(stream_key, shape, jnp.float32)
    if cuts:
        values = values * levels(stream_key, shape, cuts, -0.22, 0.18)
    return jnp.clip(values, -bound, bound).astype(kind)


def setup_inputs(seed: int = 0) -> dict:
    splits = jax.random.split(jax.random.key(seed), 9)
    return {
        "hidden_state": bell_draw(splits[0], (SEQS, D), 1.0, 6.0, ((0, 16),)),
        "lengths": draw_lengths(jax.random.fold_in(splits[8], 71), 0),
        "old_qkv": bell_draw(splits[2], (D, COLS), D ** -0.5, 0.09375, ((1, 8),)),
        "old_out": bell_draw(splits[3], (HQ * HD, D), (HQ * HD) ** -0.5, 0.09375, ((1, 8),)),
        "cache_keys": draw_cache_keys(jax.random.fold_in(splits[8], 71), 0),
        "cache_values": bell_draw(splits[5], (SEQS, CACHE_LEN, KVH * HD), 1.0, 6.0, ((0, 16), (1, 8))),
        "new_qkv": bell_draw(splits[6], (D, COLS), D ** -0.5, 0.09375, ((0, 128),)),
        "new_out": bell_draw(splits[7], (HQ * HD, D), (HQ * HD) ** -0.5, 0.09375, ((0, 128),)),
    }


ROPE_BASE = 1000000.0

def rotate(vectors, positions):
    half_dim = vectors.shape[-1] // 2
    frequency = ROPE_BASE ** (-2.0 * jnp.arange(half_dim, dtype=jnp.float32) / (2 * half_dim))
    angles = positions.astype(jnp.float32)[:, None, None] * frequency
    first_half = vectors[..., :half_dim]
    second_half = vectors[..., half_dim:]
    return jnp.concatenate([first_half * jnp.cos(angles) - second_half * jnp.sin(angles), second_half * jnp.cos(angles) + first_half * jnp.sin(angles)], axis=-1)

def reference(hidden_state, lengths, old_qkv, old_out, cache_keys, cache_values, new_qkv, new_out):
    joined = jnp.dot(hidden_state, old_qkv, preferred_element_type=jnp.float32).astype(jnp.bfloat16)
    q_width = HQ * HD
    k_width = KVH * HD
    queries = rotate(joined[:, :q_width].astype(jnp.float32).reshape(SEQS, HQ, HD), lengths).astype(jnp.bfloat16)
    own_keys = rotate(joined[:, q_width:q_width + k_width].astype(jnp.float32).reshape(SEQS, KVH, HD), lengths).astype(jnp.bfloat16)
    own_values = joined[:, q_width + k_width:].reshape(SEQS, KVH, HD)
    group_size = HQ // KVH
    inv_root = 1.0 / jnp.sqrt(jnp.float32(HD))

    def attend(per_sequence):
        query_row, own_key, own_value, length, seq_keys, seq_values = per_sequence
        grouped = query_row.reshape(KVH, group_size, HD).astype(jnp.float32)
        key_blocks = seq_keys.reshape(CACHE_LEN, KVH, HD).astype(jnp.float32)
        value_blocks = seq_values.reshape(CACHE_LEN, KVH, HD).astype(jnp.float32)
        scores = jnp.einsum('kgd,tkd->kgt', grouped, key_blocks) * inv_root
        live_mask = jnp.arange(CACHE_LEN, dtype=jnp.int32) < length
        scores = jnp.where(live_mask, scores, jnp.float32(-1e+30))
        own_score = lax.optimization_barrier(jnp.sum(grouped * own_key.astype(jnp.float32)[:, None, :], axis=-1)) * inv_root
        top_score = jnp.maximum(lax.optimization_barrier(jnp.max(scores, axis=-1)), own_score)
        weights = jnp.where(live_mask, jnp.exp(scores - top_score[..., None]), jnp.float32(0.0)).astype(jnp.bfloat16)
        own_weight = lax.optimization_barrier(jnp.exp(own_score - top_score).astype(jnp.bfloat16)).astype(jnp.float32)
        numerator = jnp.einsum('kgt,tkd->kgd', weights.astype(jnp.float32), value_blocks)
        numerator = numerator + own_weight[..., None] * own_value.astype(jnp.float32)[:, None, :]
        denominator = lax.optimization_barrier(jnp.sum(weights.astype(jnp.float32), axis=-1)) + own_weight
        return (numerator / denominator[..., None]).reshape(HQ * HD).astype(jnp.bfloat16)
    attended = lax.map(attend, (queries, own_keys, own_values, lengths, cache_keys, cache_values))
    decoded = jnp.dot(attended, old_out, preferred_element_type=jnp.float32).astype(jnp.bfloat16)
    return (decoded, new_qkv, new_out)
```

```python
import functools

import jax
import jax.numpy as jnp
from jax import lax
from jax.experimental import pallas as pl
from jax.experimental.pallas import tpu as pltpu
from jax.sharding import PartitionSpec as P

HQ = 28
KVH = 4
HD = 128
GROUP = HQ // KVH
ROPE_BASE = 1000000.0
ROWS = 28
QC = 576
OC = 448
TILES = 8
SLOT = ROWS * TILES
SEQ = 4
CHUNK = 512
PAIRS = SEQ * KVH

ITEMS = ((0, 0), (0, 1), (1, 0), (3, 0), (1, 1), (3, 1), (2, 0), (2, 1))
X_FIRST = (True, True, False, True, False, True, False, True)
F32 = jnp.float32
BF16 = jnp.bfloat16


def move_kernel(
    len_smem, hidden, trig, old_qkv, old_out, keys, values, new_qkv, new_out,
    land, decoded,
    packed, nq, no, hid, trg, wq, wo, kb, vb,
    jown, jall, jfull, qf, ownb, part, parts, att, amat, lensem,
    load_sem, recv_sem, send_sem, small_recv, small_send,
):
    rep = lax.axis_index("rep")
    tp = lax.axis_index("tp")
    core = rep % 2
    x_lo = (rep // 2) % 2
    z = rep // 4
    y = tp // 2
    x_hi = tp % 2
    z_up = (z + 1) % 4
    z_dn = (z + 3) % 4
    z_op = (z + 2) % 4
    x_ot = 1 - x_lo

    def rep_of(zz, xx, cc):
        return (zz * 2 + xx) * 2 + cc

    loads = []
    for n, (src, dst) in enumerate(
        ((new_qkv, nq), (new_out, no), (hidden, hid), (trig, trg), (old_qkv, wq), (keys, kb), (values, vb), (old_out, wo))
    ):
        c = pltpu.make_async_copy(src, dst, load_sem.at[n])
        c.start()
        loads.append(c)

    barrier = pltpu.get_barrier_semaphore()
    friends = []
    for dy in range(4):
        for f in range(2):
            t = ((y + dy) % 4) * 2 + (x_hi + f) % 2
            if (dy, f) != (0, 0):
                friends.append((rep, t))
            if f == 1:
                friends.append((rep_of(z, x_ot, core), t))
    friends.append((rep_of(z, x_ot, core), tp))
    friends.append((rep_of(z_up, x_lo, core), tp))
    friends.append((rep_of(z_dn, x_lo, core), tp))
    friends.append((rep_of(z, x_lo, 1 - core), tp))
    for r, t in friends:
        pl.semaphore_signal(barrier, inc=1, device_id={"rep": r, "tp": t}, device_id_type=pl.DeviceIdType.MESH)

    loads[0].wait()
    loads[1].wait()
    for t in range(8):
        a = nq[:, QC * t : QC * (t + 1)]
        b = no[:, OC * t : OC * (t + 1)]
        for k in range(TILES):
            if k < 4:
                v = a[:, 128 * k : 128 * (k + 1)]
            elif k == 4:
                v = jnp.concatenate([a[:, 512:576], b[:, 384:448]], axis=1)
            else:
                v = b[:, 128 * (k - 5) : 128 * (k - 4)]
            packed[t, ROWS * k : ROWS * (k + 1), :] = v
    mine = rep * 8 + tp
    land[mine] = packed[tp]
    pl.semaphore_wait(barrier, len(friends))

    sent = []

    def put(src, slot, r, t):
        c = pltpu.make_async_remote_copy(
            src_ref=src, dst_ref=land.at[slot], send_sem=send_sem.at[len(sent)], recv_sem=recv_sem.at[slot],
            device_id={"rep": r, "tp": t}, device_id_type=pl.DeviceIdType.MESH,
        )
        c.start()
        sent.append(c)

    def arrived(slot):
        pltpu.make_async_remote_copy(
            src_ref=land.at[slot], dst_ref=land.at[slot], send_sem=send_sem.at[0], recv_sem=recv_sem.at[slot],
            device_id={"rep": rep, "tp": tp}, device_id_type=pl.DeviceIdType.MESH,
        ).wait_recv()

    def slot_of(zz, xx, item):
        dy, f = item
        r = rep_of(zz, (xx + f) % 2, core)
        t = ((y + dy) % 4) * 2 + (x_hi + f) % 2
        return r * 8 + t

    def exchange():
        for dy, f in ITEMS[1:]:
            t = ((y + 4 - dy) % 4) * 2 + (x_hi + f) % 2
            put(packed.at[t], mine, rep_of(z, (x_lo + f) % 2, core), t)

    def up(slot):
        put(land.at[slot], slot, rep_of(z_up, x_lo, core), tp)

    def down(slot):
        put(land.at[slot], slot, rep_of(z_dn, x_lo, core), tp)

    def across(slot):
        put(land.at[slot], slot, rep_of(z, x_ot, core), tp)

    def twin(slot):
        put(land.at[slot], slot, rep_of(z, x_lo, 1 - core), tp)

    def step(s):
        if 0 <= s < 8:
            b = slot_of(z, x_lo, ITEMS[s])
            if s:
                arrived(b)
            across(b)
            up(b)
            down(b)
            twin(b)
        j = s - 1
        if 0 <= j < 8:
            it = ITEMS[j]
            b = slot_of(z, x_ot, it)
            arrived(b)
            if X_FIRST[j]:
                up(b)
                down(b)
            twin(b)
            for zz, go, fwd in ((z_dn, up, j % 2 == 0), (z_up, down, j % 2 == 1)):
                b = slot_of(zz, x_lo, it)
                arrived(b)
                if fwd:
                    go(b)
                if not X_FIRST[j]:
                    across(b)
                twin(b)
        j = s - 2
        if 0 <= j < 8:
            it = ITEMS[j]
            for zz, go, fwd in ((z_dn, up, j % 2 == 1), (z_up, down, j % 2 == 0)):
                b = slot_of(zz, x_ot, it)
                arrived(b)
                if fwd and X_FIRST[j]:
                    go(b)
                twin(b)
            b = slot_of(z_op, x_lo, it)
            arrived(b)
            if not X_FIRST[j]:
                across(b)
            twin(b)
        j = s - 3
        if 0 <= j < 8:
            b = slot_of(z_op, x_ot, ITEMS[j])
            arrived(b)
            twin(b)

    small = []

    def to_peers(phase, src_of, dst_of):
        for n in range(1, 8):
            t = (tp + n) % 8
            c = pltpu.make_async_remote_copy(
                src_ref=src_of(t), dst_ref=dst_of(), send_sem=small_send.at[phase, n - 1],
                recv_sem=small_recv.at[phase, tp],
                device_id={"rep": rep, "tp": t}, device_id_type=pl.DeviceIdType.MESH,
            )
            c.start()
            small.append(c)

    def from_peers(phase, dst_from):
        for n in range(1, 8):
            t = (tp + 8 - n) % 8
            pltpu.make_async_remote_copy(
                src_ref=dst_from(t), dst_ref=dst_from(t), send_sem=small_send.at[phase, 0],
                recv_sem=small_recv.at[phase, t],
                device_id={"rep": rep, "tp": tp}, device_id_type=pl.DeviceIdType.MESH,
            ).wait_recv()

    def project():
        loads[2].wait()
        loads[4].wait()
        res = jnp.dot(hid[...], wq[...], preferred_element_type=F32).astype(BF16)
        jown[0:SEQ, 0:QC] = res
        jall[tp, 0:SEQ, 0:QC] = res
        to_peers(0, lambda t: jown, lambda: jall.at[tp])

    def rotary():
        from_peers(0, lambda t: jall.at[t])
        loads[3].wait()
        for t in range(8):
            jfull[0:SEQ, QC * t : QC * (t + 1)] = jall[t, 0:SEQ, 0:QC].astype(F32)
        cos2 = trg[0:SEQ, :]
        sin2 = trg[8 : 8 + SEQ, :]
        for h in range(HQ + KVH):
            x = jfull[0:SEQ, HD * h : HD * (h + 1)]
            r = x * cos2 + pltpu.roll(x, HD // 2, 1) * sin2
            qf[8 * h : 8 * h + SEQ, :] = r.astype(BF16).astype(F32)
        inv_root = 1.0 / jnp.sqrt(F32(HD))
        for s in range(SEQ):
            for k in range(KVH):
                q = qf[pl.ds(8 * GROUP * k + s, 8, stride=8), :]
                key = qf[8 * (HQ + k) + s : 8 * (HQ + k) + s + 1, :]
                own = jnp.sum(q * key, axis=1, keepdims=True) * inv_root
                ownb[s * KVH + k, 0:8, :] = jnp.broadcast_to(own, (8, HD))
                c0 = HQ * HD + KVH * HD + HD * k
                ownb[s * KVH + k, 8:16, :] = jnp.broadcast_to(jfull[s : s + 1, c0 : c0 + HD], (8, HD))

    def attend(s):
        if s == 0:
            loads[5].wait()
            loads[6].wait()
        inv_root = 1.0 / jnp.sqrt(F32(HD))
        pos = lax.broadcasted_iota(jnp.int32, (8, CHUNK), 1) + tp * CHUNK
        live = pos < len_smem[s]
        lane = lax.broadcasted_iota(jnp.int32, (8, HD), 1)
        for k in range(KVH):
            q = qf[pl.ds(8 * GROUP * k + s, 8, stride=8), :].astype(BF16)
            sc = lax.dot_general(
                q, kb[s, :, HD * k : HD * (k + 1)], (((1,), (1,)), ((), ())), preferred_element_type=F32
            ) * inv_root
            sc = jnp.where(live, sc, F32(-1e30))
            m = jnp.max(sc, axis=1, keepdims=True)
            p = jnp.where(live, jnp.exp(sc - m), F32(0.0)).astype(BF16)
            l = jnp.sum(p.astype(F32), axis=1, keepdims=True)
            n = jnp.dot(p, vb[s, :, HD * k : HD * (k + 1)], preferred_element_type=F32)
            part[s * KVH + k, 0:8, :] = n
            part[s * KVH + k, 8:16, :] = jnp.where(
                lane == 0, jnp.broadcast_to(m, (8, HD)), jnp.broadcast_to(l, (8, HD))
            )

    def share():
        parts[tp] = part[pl.ds(2 * tp, 2)]
        to_peers(1, lambda t: part.at[pl.ds(2 * t, 2)], lambda: parts.at[tp])

    def combine():
        from_peers(1, lambda t: parts.at[t])
        for n in range(2):
            own = ownb[2 * tp + n, 0:8, :]
            val = ownb[2 * tp + n, 8:16, :]
            top = own
            for t in range(8):
                top = jnp.maximum(top, jnp.broadcast_to(parts[t, n, 8:16, 0:1], (8, HD)))
            w = jnp.exp(own - top).astype(BF16).astype(F32)
            num = w * val
            den = w
            for t in range(8):
                scale = jnp.exp(jnp.broadcast_to(parts[t, n, 8:16, 0:1], (8, HD)) - top)
                num = num + parts[t, n, 0:8, :] * scale
                den = den + jnp.broadcast_to(parts[t, n, 8:16, 1:2], (8, HD)) * scale
            att[2 * tp + n] = (num / den).astype(BF16).astype(F32)
        to_peers(2, lambda t: att.at[pl.ds(2 * tp, 2)], lambda: att.at[pl.ds(2 * tp, 2)])

    def finish():
        from_peers(2, lambda t: att.at[pl.ds(2 * t, 2)])
        loads[7].wait()
        for k in range(KVH):
            for g in range(GROUP):
                h = GROUP * k + g
                for s in range(SEQ):
                    amat[s : s + 1, HD * h : HD * (h + 1)] = att[s * KVH + k, g : g + 1, :]
        decoded[...] = jnp.dot(
            amat[0:SEQ, :].astype(BF16), wo[...], preferred_element_type=F32
        ).astype(BF16)

    step(0)
    exchange()
    project()
    step(1)
    step(2)
    rotary()
    step(3)
    attend(0)
    attend(1)
    step(4)
    attend(2)
    attend(3)
    share()
    step(5)
    step(6)
    combine()
    step(7)
    step(8)
    finish()
    step(9)
    step(10)
    for it in ITEMS:
        for zz in (z, z_dn, z_up, z_op):
            for xx in (x_lo, x_ot):
                b = slot_of(zz, xx, it)
                arrived(b + 8 * (1 - 2 * core))
    for c in sent:
        c.wait_send()
    for c in small:
        c.wait_send()


def write_kernel(land, dec, out_q, out_o, out_d, oq, oo, sems):
    parts = 8
    rows = 3584 // parts
    copies = []
    d = pltpu.make_async_copy(dec, out_d, sems.at[2 * parts])
    d.start()
    for p in range(parts):

        def body(i, _):
            r0 = pl.multiple_of(p * rows + i * 112, 112)
            tq = oq.at[pl.ds(r0, 112)]
            to = oo.at[pl.ds(r0, 112)]
            for m in range(4):
                b = p * 16 + i * 4 + m
                for k in range(TILES):
                    v = land[b, ROWS * k : ROWS * (k + 1), :]
                    at = pl.ds(ROWS * m, ROWS)
                    if k < 4:
                        tq[at, 128 * k : 128 * (k + 1)] = v
                    elif k == 4:
                        tq[at, 512:576] = v[:, 0:64]
                        to[at, 384:448] = v[:, 64:128]
                    else:
                        to[at, 128 * (k - 5) : 128 * (k - 4)] = v
            return 0

        lax.fori_loop(0, rows // 112, body, 0)
        for n, (src, dst) in enumerate(((oq, out_q), (oo, out_o))):
            c = pltpu.make_async_copy(src.at[pl.ds(p * rows, rows)], dst.at[pl.ds(p * rows, rows)], sems.at[2 * p + n])
            c.start()
            copies.append(c)
    for c in copies:
        c.wait()
    d.wait()


def per_device(hidden_state, lengths, old_qkv, old_out, cache_keys, cache_values, new_qkv, new_out):
    half = HD // 2
    frequency = ROPE_BASE ** (-2.0 * jnp.arange(half, dtype=F32) / (2 * half))
    angles = lengths.astype(F32)[:, None] * frequency
    cos, sin = jnp.cos(angles), jnp.sin(angles)
    pad = jnp.zeros((4, HD), F32)
    trig = jnp.concatenate(
        [jnp.concatenate([cos, cos], 1), pad, jnp.concatenate([-sin, sin], 1), pad], 0
    )
    any_ = pl.BlockSpec(memory_space=pl.ANY)
    vmem = pl.BlockSpec(memory_space=pltpu.VMEM)
    land, dec = pl.pallas_call(
        move_kernel,
        out_shape=(pltpu.VMEM((128, SLOT, 128), BF16), pltpu.VMEM((SEQ, OC), BF16)),
        in_specs=[pl.BlockSpec(memory_space=pltpu.SMEM)] + [any_] * 8,
        out_specs=(vmem, vmem),
        scratch_shapes=[
            pltpu.VMEM((8, SLOT, 128), BF16),
            pltpu.VMEM((ROWS, 4608), BF16),
            pltpu.VMEM((ROWS, 3584), BF16),
            pltpu.VMEM((SEQ, 3584), BF16),
            pltpu.VMEM((16, HD), F32),
            pltpu.VMEM((3584, QC), BF16),
            pltpu.VMEM((3584, OC), BF16),
            pltpu.VMEM((SEQ, CHUNK, 512), BF16),
            pltpu.VMEM((SEQ, CHUNK, 512), BF16),
            pltpu.VMEM((16, 640), BF16),
            pltpu.VMEM((8, 16, 640), BF16),
            pltpu.VMEM((8, 4608), F32),
            pltpu.VMEM((8 * (HQ + KVH), HD), F32),
            pltpu.VMEM((PAIRS, 16, HD), F32),
            pltpu.VMEM((PAIRS, 16, HD), F32),
            pltpu.VMEM((8, 2, 16, HD), F32),
            pltpu.VMEM((PAIRS, 8, HD), F32),
            pltpu.VMEM((8, 3584), F32),
            pltpu.SemaphoreType.REGULAR,
            pltpu.SemaphoreType.DMA((8,)),
            pltpu.SemaphoreType.DMA((128,)),
            pltpu.SemaphoreType.DMA((128,)),
            pltpu.SemaphoreType.DMA((3, 8)),
            pltpu.SemaphoreType.DMA((3, 7)),
        ],
        compiler_params=pltpu.CompilerParams(
            collective_id=0, has_side_effects=True, vmem_limit_bytes=40 * 1024 * 1024
        ),
        name="move",
    )(lengths, hidden_state, trig, old_qkv, old_out, cache_keys, cache_values, new_qkv, new_out)
    qkv_tp, out_tp, decoded = pl.pallas_call(
        write_kernel,
        out_shape=(
            jax.ShapeDtypeStruct((3584, QC), BF16),
            jax.ShapeDtypeStruct((3584, OC), BF16),
            jax.ShapeDtypeStruct((SEQ, OC), BF16),
        ),
        in_specs=[vmem, vmem],
        out_specs=(any_, any_, any_),
        scratch_shapes=[
            pltpu.VMEM((3584, QC), BF16),
            pltpu.VMEM((3584, OC), BF16),
            pltpu.SemaphoreType.DMA((17,)),
        ],
        compiler_params=pltpu.CompilerParams(vmem_limit_bytes=24 * 1024 * 1024),
        name="write",
    )(land, dec)
    return decoded, qkv_tp, out_tp


def solution(mesh):
    in_specs = (
        P("rep", None),
        P("rep"),
        P(None, "tp"),
        P(None, "tp"),
        P("rep", "tp", None),
        P("rep", "tp", None),
        P(("rep", "tp"), None),
        P(("rep", "tp"), None),
    )
    out_specs = (P("rep", "tp"), P(None, "tp"), P(None, "tp"))
    return jax.shard_map(per_device, mesh=mesh, in_specs=in_specs, out_specs=out_specs, check_vma=False)
```

```python
import jax
import jax.numpy as jnp
import numpy as np
from jax import lax
from jax.experimental import pallas as pl
from jax.experimental.pallas import tpu as pltpu
from jax.sharding import PartitionSpec as P

HQ = 28
KVH = 4
HD = 128
GROUP = HQ // KVH
ROPE_BASE = 1000000.0
ROWS = 28
QC = 576
OC = 448
TILES = 8
QUADS = ROWS // 4
SEQ = 4
CHUNK = 512
PAIRS = SEQ * KVH

ITEMS = ((0, 0), (0, 1), (1, 0), (3, 0), (1, 1), (3, 1), (2, 0), (2, 1))
X_FIRST = (True, True, False, True, False, True, False, True)
F32 = jnp.float32
BF16 = jnp.bfloat16
NT = (((1,), (1,)), ((), ()))


def move_kernel(
    len_smem, hidden, freq, old_qkv, old_out, keys, values, new_qkv, new_out,
    land, decoded,
    packed, nq, no, hid, frq, wq, wo, kb, vb,
    jown, jall, jfull, qf, ownb, part, parts, att, amat,
    load_sem, recv_sem, send_sem, small_recv, small_send,
):
    rep = lax.axis_index("rep")
    tp = lax.axis_index("tp")
    core = rep % 2
    x_lo = (rep // 2) % 2
    z = rep // 4
    y = tp // 2
    x_hi = tp % 2
    z_up = (z + 1) % 4
    z_dn = (z + 3) % 4
    z_op = (z + 2) % 4
    x_ot = 1 - x_lo

    def rep_of(zz, xx, cc):
        return (zz * 2 + xx) * 2 + cc

    loads = []
    for n, (src, dst) in enumerate(
        ((new_qkv, nq), (new_out, no), (hidden, hid), (freq, frq), (old_qkv, wq), (keys, kb), (values, vb), (old_out, wo))
    ):
        c = pltpu.make_async_copy(src, dst, load_sem.at[n])
        c.start()
        loads.append(c)

    barrier = pltpu.get_barrier_semaphore()
    friends = []
    for dy in range(4):
        for f in range(2):
            t = ((y + dy) % 4) * 2 + (x_hi + f) % 2
            if (dy, f) != (0, 0):
                friends.append((rep, t))
            if f == 1:
                friends.append((rep_of(z, x_ot, core), t))
    friends.append((rep_of(z, x_ot, core), tp))
    friends.append((rep_of(z_up, x_lo, core), tp))
    friends.append((rep_of(z_dn, x_lo, core), tp))
    friends.append((rep_of(z, x_lo, 1 - core), tp))
    for r, t in friends:
        pl.semaphore_signal(barrier, inc=1, device_id={"rep": r, "tp": t}, device_id_type=pl.DeviceIdType.MESH)

    loads[0].wait()
    loads[1].wait()
    for t in range(8):
        a = nq[:, QC * t : QC * (t + 1)]
        b = no[:, OC * t : OC * (t + 1)]
        for k in range(TILES):
            if k < 4:
                v = a[:, 128 * k : 128 * (k + 1)]
            elif k == 4:
                v = jnp.concatenate([a[:, 512:576], b[:, 384:448]], axis=1)
            else:
                v = b[:, 128 * (k - 5) : 128 * (k - 4)]
            packed[t, k] = v.reshape(QUADS, 4, 128)
    mine = rep * 8 + tp
    land[:, pl.ds(QUADS * mine, QUADS)] = packed[tp]
    pl.semaphore_wait(barrier, len(friends))

    sent = []

    def place(slot):
        return land.at[:, pl.ds(QUADS * slot, QUADS)]

    def put(src, slot, r, t):
        c = pltpu.make_async_remote_copy(
            src_ref=src, dst_ref=place(slot), send_sem=send_sem.at[len(sent)], recv_sem=recv_sem.at[slot],
            device_id={"rep": r, "tp": t}, device_id_type=pl.DeviceIdType.MESH,
        )
        c.start()
        sent.append(c)

    def arrived(slot):
        pltpu.make_async_remote_copy(
            src_ref=place(slot), dst_ref=place(slot), send_sem=send_sem.at[0], recv_sem=recv_sem.at[slot],
            device_id={"rep": rep, "tp": tp}, device_id_type=pl.DeviceIdType.MESH,
        ).wait_recv()

    def slot_of(zz, xx, item):
        dy, f = item
        r = rep_of(zz, (xx + f) % 2, core)
        t = ((y + dy) % 4) * 2 + (x_hi + f) % 2
        return r * 8 + t

    def exchange():
        for dy, f in ITEMS[1:]:
            t = ((y + 4 - dy) % 4) * 2 + (x_hi + f) % 2
            put(packed.at[t], mine, rep_of(z, (x_lo + f) % 2, core), t)

    def up(slot):
        put(place(slot), slot, rep_of(z_up, x_lo, core), tp)

    def down(slot):
        put(place(slot), slot, rep_of(z_dn, x_lo, core), tp)

    def across(slot):
        put(place(slot), slot, rep_of(z, x_ot, core), tp)

    def twin(slot):
        put(place(slot), slot, rep_of(z, x_lo, 1 - core), tp)

    def step(s):
        if 0 <= s < 8:
            b = slot_of(z, x_lo, ITEMS[s])
            if s:
                arrived(b)
            across(b)
            up(b)
            down(b)
            twin(b)
        j = s - 1
        if 0 <= j < 8:
            it = ITEMS[j]
            b = slot_of(z, x_ot, it)
            arrived(b)
            if X_FIRST[j]:
                up(b)
                down(b)
            twin(b)
            for zz, go, fwd in ((z_dn, up, j % 2 == 0), (z_up, down, j % 2 == 1)):
                b = slot_of(zz, x_lo, it)
                arrived(b)
                if fwd:
                    go(b)
                if not X_FIRST[j]:
                    across(b)
                twin(b)
        j = s - 2
        if 0 <= j < 8:
            it = ITEMS[j]
            for zz, go, fwd in ((z_dn, up, j % 2 == 1), (z_up, down, j % 2 == 0)):
                b = slot_of(zz, x_ot, it)
                arrived(b)
                if fwd and X_FIRST[j]:
                    go(b)
                twin(b)
            b = slot_of(z_op, x_lo, it)
            arrived(b)
            if not X_FIRST[j]:
                across(b)
            twin(b)
        j = s - 3
        if 0 <= j < 8:
            b = slot_of(z_op, x_ot, ITEMS[j])
            arrived(b)
            twin(b)

    small = []

    def to_peers(phase, src_of, dst_of):
        for n in range(1, 8):
            t = (tp + n) % 8
            c = pltpu.make_async_remote_copy(
                src_ref=src_of(t), dst_ref=dst_of(), send_sem=small_send.at[phase, n - 1],
                recv_sem=small_recv.at[phase, tp],
                device_id={"rep": rep, "tp": t}, device_id_type=pl.DeviceIdType.MESH,
            )
            c.start()
            small.append(c)

    def from_peers(phase, dst_from):
        for n in range(1, 8):
            t = (tp + 8 - n) % 8
            pltpu.make_async_remote_copy(
                src_ref=dst_from(t), dst_ref=dst_from(t), send_sem=small_send.at[phase, 0],
                recv_sem=small_recv.at[phase, t],
                device_id={"rep": rep, "tp": tp}, device_id_type=pl.DeviceIdType.MESH,
            ).wait_recv()

    def project():
        loads[2].wait()
        loads[4].wait()
        res = lax.dot_general(hid[...], wq[...], NT, preferred_element_type=F32).astype(BF16)
        jown[0:SEQ, 0:QC] = res
        jall[tp, 0:SEQ, 0:QC] = res
        to_peers(0, lambda t: jown, lambda: jall.at[tp])

    def rotary():
        from_peers(0, lambda t: jall.at[t])
        loads[3].wait()
        row = lax.broadcasted_iota(jnp.int32, (8, HD), 0)
        lane = lax.broadcasted_iota(jnp.int32, (8, HD), 1)
        pos = jnp.zeros((8, HD), F32)
        for s in range(SEQ):
            pos = jnp.where(row == s, len_smem[s].astype(F32), pos)
        angles = pos * jnp.broadcast_to(frq[0:1, :], (8, HD))
        cos2 = jnp.cos(angles)[0:SEQ]
        sin2 = jnp.where(lane < HD // 2, -jnp.sin(angles), jnp.sin(angles))[0:SEQ]
        for t in range(8):
            jfull[0:SEQ, QC * t : QC * (t + 1)] = jall[t, 0:SEQ, 0:QC].astype(F32)
        for h in range(HQ + KVH):
            x = jfull[0:SEQ, HD * h : HD * (h + 1)]
            r = x * cos2 + pltpu.roll(x, HD // 2, 1) * sin2
            qf[8 * h : 8 * h + SEQ, :] = r.astype(BF16).astype(F32)
        inv_root = 1.0 / jnp.sqrt(F32(HD))
        for s in range(SEQ):
            for k in range(KVH):
                q = qf[pl.ds(8 * GROUP * k + s, 8, stride=8), :]
                key = qf[8 * (HQ + k) + s : 8 * (HQ + k) + s + 1, :]
                own = jnp.sum(q * key, axis=1, keepdims=True) * inv_root
                ownb[s * KVH + k, 0:8, :] = jnp.broadcast_to(own, (8, HD))
                c0 = HQ * HD + KVH * HD + HD * k
                ownb[s * KVH + k, 8:16, :] = jnp.broadcast_to(jfull[s : s + 1, c0 : c0 + HD], (8, HD))

    def attend(s):
        if s == 0:
            loads[5].wait()
            loads[6].wait()
        inv_root = 1.0 / jnp.sqrt(F32(HD))
        pos = lax.broadcasted_iota(jnp.int32, (8, CHUNK), 1) + tp * CHUNK
        live = pos < len_smem[s]
        lane = lax.broadcasted_iota(jnp.int32, (8, HD), 1)
        for k in range(KVH):
            q = qf[pl.ds(8 * GROUP * k + s, 8, stride=8), :].astype(BF16)
            sc = lax.dot_general(
                q, kb[s, :, HD * k : HD * (k + 1)], NT, preferred_element_type=F32
            ) * inv_root
            sc = jnp.where(live, sc, F32(-1e30))
            m = jnp.max(sc, axis=1, keepdims=True)
            p = jnp.where(live, jnp.exp(sc - m), F32(0.0)).astype(BF16)
            l = jnp.sum(p.astype(F32), axis=1, keepdims=True)
            n = jnp.dot(p, vb[s, :, HD * k : HD * (k + 1)], preferred_element_type=F32)
            part[s * KVH + k, 0:8, :] = n
            part[s * KVH + k, 8:16, :] = jnp.where(
                lane == 0, jnp.broadcast_to(m, (8, HD)), jnp.broadcast_to(l, (8, HD))
            )

    def share():
        parts[tp] = part[pl.ds(2 * tp, 2)]
        to_peers(1, lambda t: part.at[pl.ds(2 * t, 2)], lambda: parts.at[tp])

    def combine():
        from_peers(1, lambda t: parts.at[t])
        for n in range(2):
            own = ownb[2 * tp + n, 0:8, :]
            val = ownb[2 * tp + n, 8:16, :]
            top = own
            for t in range(8):
                top = jnp.maximum(top, jnp.broadcast_to(parts[t, n, 8:16, 0:1], (8, HD)))
            w = jnp.exp(own - top).astype(BF16).astype(F32)
            num = w * val
            den = w
            for t in range(8):
                scale = jnp.exp(jnp.broadcast_to(parts[t, n, 8:16, 0:1], (8, HD)) - top)
                num = num + parts[t, n, 0:8, :] * scale
                den = den + jnp.broadcast_to(parts[t, n, 8:16, 1:2], (8, HD)) * scale
            att[2 * tp + n] = (num / den).astype(BF16).astype(F32)
        to_peers(2, lambda t: att.at[pl.ds(2 * tp, 2)], lambda: att.at[pl.ds(2 * tp, 2)])

    def finish():
        from_peers(2, lambda t: att.at[pl.ds(2 * t, 2)])
        loads[7].wait()
        for k in range(KVH):
            for g in range(GROUP):
                h = GROUP * k + g
                for s in range(SEQ):
                    amat[s : s + 1, HD * h : HD * (h + 1)] = att[s * KVH + k, g : g + 1, :]
        decoded[...] = lax.dot_general(
            amat[0:SEQ, :].astype(BF16), wo[...], NT, preferred_element_type=F32
        ).astype(BF16)

    step(0)
    exchange()
    project()
    step(1)
    step(2)
    rotary()
    step(3)
    attend(0)
    attend(1)
    step(4)
    attend(2)
    attend(3)
    share()
    step(5)
    step(6)
    combine()
    step(7)
    step(8)
    finish()
    step(9)
    step(10)
    for it in ITEMS:
        for zz in (z, z_dn, z_up, z_op):
            for xx in (x_lo, x_ot):
                b = slot_of(zz, xx, it)
                arrived(b + 8 * (1 - 2 * core))
    for c in sent:
        c.wait_send()
    for c in small:
        c.wait_send()


def write_kernel(land, dec, out_q, out_o, out_d, oq, oo, sems):
    eye = jnp.where(
        lax.broadcasted_iota(jnp.int32, (256, 256), 0) == lax.broadcasted_iota(jnp.int32, (256, 256), 1), 1.0, 0.0
    ).astype(BF16)
    copies = []

    def out(src, dst, first, n):
        c = pltpu.make_async_copy(src.at[pl.ds(first, n)], dst.at[pl.ds(first, n)], sems.at[len(copies)])
        c.start()
        copies.append(c)

    d = pltpu.make_async_copy(dec, out_d, sems.at[6])
    d.start()
    for c in range(4):

        def body(i, _):
            q0 = i * 64
            w = jnp.concatenate(
                [land[2 * c + n, pl.ds(q0, 64)].reshape(256, 128) for n in range(2)], axis=1
            )
            v = lax.dot_general(eye, w, NT, preferred_element_type=F32).astype(BF16)
            at = pl.ds(pl.multiple_of(i * 256, 256), 256)
            if c < 2:
                oq[256 * c : 256 * (c + 1), at] = v
            elif c == 2:
                oq[512:576, at] = v[0:64]
                oo[384:448, at] = v[64:128]
                oo[0:128, at] = v[128:256]
            else:
                oo[128:384, at] = v
            return 0

        lax.fori_loop(0, 14, body, 0)
        if c < 2:
            out(oq, out_q, 256 * c, 256)
        elif c == 2:
            out(oq, out_q, 512, 64)
            out(oo, out_o, 384, 64)
            out(oo, out_o, 0, 128)
        else:
            out(oo, out_o, 128, 256)
    for c in copies:
        c.wait()
    d.wait()


def per_device(hidden_state, lengths, old_qkv, old_out, cache_keys, cache_values, new_qkv, new_out):
    half = ROPE_BASE ** (-2.0 * np.arange(HD // 2) / HD)
    freq = jnp.asarray(np.concatenate([half, half])[None], F32)
    any_ = pl.BlockSpec(memory_space=pl.ANY)
    hbm = pl.BlockSpec(memory_space=pltpu.HBM)
    vmem = pl.BlockSpec(memory_space=pltpu.VMEM)
    far = [
        pltpu.with_memory_space_constraint(a, pltpu.HBM)
        for a in (hidden_state, freq, old_qkv.T, old_out.T, cache_keys, cache_values, new_qkv, new_out)
    ]
    land, dec = pl.pallas_call(
        move_kernel,
        out_shape=(pltpu.VMEM((TILES, 128 * QUADS, 4, 128), BF16), pltpu.VMEM((SEQ, OC), BF16)),
        in_specs=[pl.BlockSpec(memory_space=pltpu.SMEM)] + [hbm] * 8,
        out_specs=(vmem, vmem),
        scratch_shapes=[
            pltpu.VMEM((8, TILES, QUADS, 4, 128), BF16),
            pltpu.VMEM((ROWS, 4608), BF16),
            pltpu.VMEM((ROWS, 3584), BF16),
            pltpu.VMEM((SEQ, 3584), BF16),
            pltpu.VMEM((1, HD), F32),
            pltpu.VMEM((QC, 3584), BF16),
            pltpu.VMEM((OC, 3584), BF16),
            pltpu.VMEM((SEQ, CHUNK, 512), BF16),
            pltpu.VMEM((SEQ, CHUNK, 512), BF16),
            pltpu.VMEM((16, 640), BF16),
            pltpu.VMEM((8, 16, 640), BF16),
            pltpu.VMEM((8, 4608), F32),
            pltpu.VMEM((8 * (HQ + KVH), HD), F32),
            pltpu.VMEM((PAIRS, 16, HD), F32),
            pltpu.VMEM((PAIRS, 16, HD), F32),
            pltpu.VMEM((8, 2, 16, HD), F32),
            pltpu.VMEM((PAIRS, 8, HD), F32),
            pltpu.VMEM((8, 3584), F32),
            pltpu.SemaphoreType.DMA((8,)),
            pltpu.SemaphoreType.DMA((128,)),
            pltpu.SemaphoreType.DMA((128,)),
            pltpu.SemaphoreType.DMA((3, 8)),
            pltpu.SemaphoreType.DMA((3, 7)),
        ],
        compiler_params=pltpu.CompilerParams(
            collective_id=0, has_side_effects=True, vmem_limit_bytes=40 * 1024 * 1024
        ),
        name="move",
    )(lengths, *far)
    qkv_tp, out_tp, decoded = pl.pallas_call(
        write_kernel,
        out_shape=(pltpu.HBM((QC, 3584), BF16), pltpu.HBM((OC, 3584), BF16), pltpu.HBM((SEQ, OC), BF16)),
        in_specs=[vmem, vmem],
        out_specs=(hbm, hbm, hbm),
        scratch_shapes=[
            pltpu.VMEM((QC, 3584), BF16),
            pltpu.VMEM((OC, 3584), BF16),
            pltpu.SemaphoreType.DMA((7,)),
        ],
        compiler_params=pltpu.CompilerParams(vmem_limit_bytes=24 * 1024 * 1024),
        name="write",
    )(land, dec)
    return decoded, qkv_tp.T, out_tp.T


def solution(mesh):
    in_specs = (
        P("rep", None),
        P("rep"),
        P(None, "tp"),
        P(None, "tp"),
        P("rep", "tp", None),
        P("rep", "tp", None),
        P(("rep", "tp"), None),
        P(("rep", "tp"), None),
    )
    out_specs = (P("rep", "tp"), P(None, "tp"), P(None, "tp"))
    return jax.shard_map(per_device, mesh=mesh, in_specs=in_specs, out_specs=out_specs, check_vma=False)
```

```python
import jax
import jax.numpy as jnp
import numpy as np
from jax import lax
from jax.experimental import pallas as pl
from jax.experimental.pallas import tpu as pltpu
from jax.sharding import PartitionSpec as P

HQ = 28
KVH = 4
HD = 128
GROUP = HQ // KVH
ROPE_BASE = 1000000.0
ROWS = 28
QC = 576
OC = 448
TILES = 8
QUADS = ROWS // 4
SEQ = 4
CHUNK = 512
PAIRS = SEQ * KVH

ITEMS = ((0, 0), (0, 1), (1, 0), (3, 0), (1, 1), (3, 1), (2, 0), (2, 1))
X_FIRST = (False, True, True, True, True, False, False, False)
ORDER = (
    ("O", 0), ("O", 1), ("P", 0), ("D", 0), ("U", 0), ("O", 2), ("O", 3), ("O", 4), ("O", 5), ("P", 1), ("D", 1),
    ("U", 1), ("O", 6), ("d", 0), ("V", 0), ("U", 2), ("O", 7), ("u", 0), ("D", 2), ("U", 3), ("P", 2), ("D", 3),
    ("U", 4), ("P", 3), ("D", 4), ("U", 5), ("P", 4), ("D", 5), ("V", 1), ("P", 5), ("d", 1), ("u", 1), ("P", 6),
    ("D", 6), ("U", 6), ("v", 0), ("D", 7), ("U", 7), ("P", 7), ("V", 2), ("V", 3), ("d", 2), ("u", 2), ("u", 5),
    ("d", 5), ("V", 4), ("V", 5), ("d", 3), ("d", 6), ("u", 3), ("d", 4), ("u", 4), ("u", 6), ("d", 7), ("v", 1),
    ("V", 7), ("v", 2), ("u", 7), ("V", 6), ("v", 3), ("v", 4), ("v", 5), ("v", 7), ("v", 6),
)
DECODE = {
    ("O", 0): ("exchange", "project"), ("U", 1): ("rotary",), ("U", 2): ("attend0",), ("U", 4): ("attend1",),
    ("P", 4): ("attend2",), ("P", 6): ("attend3", "share"), ("V", 5): ("combine",), ("d", 7): ("finish",),
}
F32 = jnp.float32
BF16 = jnp.bfloat16
NT = (((1,), (1,)), ((), ()))


def move_kernel(
    lengths, hidden, freq, old_qkv, old_out, keys, values, new_qkv, new_out,
    land, decoded,
    packed, nq, no, hid, frq, wq, wo, kb, vb,
    jown, jall, jfull, qf, ownb, part, parts, att, amat,
    lens, load_sem, recv_sem, twin_sem, send_sem, small_recv, small_send,
):
    rep = lax.axis_index("rep")
    tp = lax.axis_index("tp")
    core = rep % 2
    x_lo = (rep // 2) % 2
    z = rep // 4
    y = tp // 2
    x_hi = tp % 2
    z_up = (z + 1) % 4
    z_dn = (z + 3) % 4
    z_op = (z + 2) % 4
    x_ot = 1 - x_lo

    def rep_of(zz, xx, cc):
        return (zz * 2 + xx) * 2 + cc

    loads = []
    for n, (src, dst) in enumerate(
        ((new_qkv, nq), (new_out, no), (hidden, hid), (freq, frq), (old_qkv, wq), (keys, kb), (values, vb), (old_out, wo), (lengths, lens))
    ):
        c = pltpu.make_async_copy(src, dst, load_sem.at[n])
        c.start()
        loads.append(c)

    barrier = pltpu.get_barrier_semaphore()
    friends = []
    for dy in range(4):
        for f in range(2):
            t = ((y + dy) % 4) * 2 + (x_hi + f) % 2
            if (dy, f) != (0, 0):
                friends.append((rep, t))
            if f == 1:
                friends.append((rep_of(z, x_ot, core), t))
    friends.append((rep_of(z, x_ot, core), tp))
    friends.append((rep_of(z_up, x_lo, core), tp))
    friends.append((rep_of(z_dn, x_lo, core), tp))
    friends.append((rep_of(z, x_lo, 1 - core), tp))
    for r, t in friends:
        pl.semaphore_signal(barrier, inc=1, device_id={"rep": r, "tp": t}, device_id_type=pl.DeviceIdType.MESH)

    loads[0].wait()
    loads[1].wait()
    for t in range(8):
        a = nq[:, QC * t : QC * (t + 1)]
        b = no[:, OC * t : OC * (t + 1)]
        for k in range(TILES):
            if k < 4:
                v = a[:, 128 * k : 128 * (k + 1)]
            elif k == 4:
                v = jnp.concatenate([a[:, 512:576], b[:, 384:448]], axis=1)
            else:
                v = b[:, 128 * (k - 5) : 128 * (k - 4)]
            packed[t, k] = v.reshape(QUADS, 4, 128)
    mine = rep * 8 + tp
    land[:, pl.ds(QUADS * mine, QUADS)] = packed[tp]
    pl.semaphore_wait(barrier, len(friends))

    sent = []

    def slot_key(slot):
        return slot // 16 * 8 + slot % 8

    def place(slot):
        return land.at[:, pl.ds(QUADS * slot, QUADS)]

    def put(src, slot, r, t, sem=None):
        c = pltpu.make_async_remote_copy(
            src_ref=src, dst_ref=place(slot), send_sem=send_sem.at[0],
            recv_sem=recv_sem.at[slot_key(slot)] if sem is None else sem,
            device_id={"rep": r, "tp": t}, device_id_type=pl.DeviceIdType.MESH,
        )
        c.start()
        sent.append(c)

    def arrived(slot):
        pltpu.make_async_remote_copy(
            src_ref=place(slot), dst_ref=place(slot), send_sem=send_sem.at[0],
            recv_sem=recv_sem.at[slot_key(slot)],
            device_id={"rep": rep, "tp": tp}, device_id_type=pl.DeviceIdType.MESH,
        ).wait_recv()

    def slot_of(zz, xx, item):
        dy, f = item
        r = rep_of(zz, (xx + f) % 2, core)
        t = ((y + dy) % 4) * 2 + (x_hi + f) % 2
        return r * 8 + t

    def exchange():
        for dy, f in ITEMS[1:]:
            t = ((y + 4 - dy) % 4) * 2 + (x_hi + f) % 2
            put(packed.at[t], mine, rep_of(z, (x_lo + f) % 2, core), t)

    def up(slot):
        put(place(slot), slot, rep_of(z_up, x_lo, core), tp)

    def down(slot):
        put(place(slot), slot, rep_of(z_dn, x_lo, core), tp)

    def across(slot):
        put(place(slot), slot, rep_of(z, x_ot, core), tp)

    def twin(slot, j):
        put(place(slot), slot, rep_of(z, x_lo, 1 - core), tp, twin_sem.at[j])

    def handle(kind, j):
        first, fwd_up = X_FIRST[j], j % 2 == 0
        zz = {"o": z, "p": z, "d": z_dn, "u": z_up, "v": z_op}[kind.lower()]
        xx = x_lo if kind in "ODUV" else x_ot
        b = slot_of(zz, xx, ITEMS[j])
        if (kind, j) != ("O", 0):
            arrived(b)
        if kind == "O" or (kind == "P" and first):
            up(b)
            down(b)
        if (kind == "D" and fwd_up) or (kind == "d" and first and not fwd_up):
            up(b)
        if (kind == "U" and not fwd_up) or (kind == "u" and first and fwd_up):
            down(b)
        if kind == "O" or (kind in "DUV" and not first):
            across(b)
        twin(b, j)

    small = []

    def to_peers(phase, src_of, dst_of):
        for n in range(1, 8):
            t = (tp + n) % 8
            c = pltpu.make_async_remote_copy(
                src_ref=src_of(t), dst_ref=dst_of(), send_sem=small_send.at[phase],
                recv_sem=small_recv.at[phase],
                device_id={"rep": rep, "tp": t}, device_id_type=pl.DeviceIdType.MESH,
            )
            c.start()
            small.append(c)

    def all_bytes(ref, sem):
        pltpu.make_async_copy(ref, ref, sem).wait()

    seven = (jall.at[pl.ds(0, 7)], parts.at[pl.ds(0, 7)], att.at[pl.ds(0, 7 * 16)])

    def project():
        loads[2].wait()
        loads[4].wait()
        res = lax.dot_general(hid[...], wq[...], NT, preferred_element_type=F32).astype(BF16)
        jown[0:SEQ, 0:QC] = res
        jall[tp, 0:SEQ, 0:QC] = res
        to_peers(0, lambda t: jown, lambda: jall.at[tp])

    def rotary():
        all_bytes(seven[0], small_recv.at[0])
        loads[3].wait()
        loads[8].wait()
        row = lax.broadcasted_iota(jnp.int32, (8, HD), 0)
        lane = lax.broadcasted_iota(jnp.int32, (8, HD), 1)
        pos = jnp.zeros((8, HD), F32)
        for s in range(SEQ):
            pos = jnp.where(row == s, lens[s].astype(F32), pos)
        angles = pos * jnp.broadcast_to(frq[0:1, :], (8, HD))
        cos2 = jnp.cos(angles)[0:SEQ]
        sin2 = jnp.where(lane < HD // 2, -jnp.sin(angles), jnp.sin(angles))[0:SEQ]
        for t in range(8):
            jfull[0:SEQ, QC * t : QC * (t + 1)] = jall[t, 0:SEQ, 0:QC].astype(F32)
        for h in range(HQ + KVH):
            x = jfull[0:SEQ, HD * h : HD * (h + 1)]
            r = x * cos2 + pltpu.roll(x, HD // 2, 1) * sin2
            qf[8 * h : 8 * h + SEQ, :] = r.astype(BF16).astype(F32)
        inv_root = 1.0 / jnp.sqrt(F32(HD))
        for s in range(SEQ):
            for k in range(KVH):
                q = qf[pl.ds(8 * GROUP * k + s, 8, stride=8), :]
                key = qf[8 * (HQ + k) + s : 8 * (HQ + k) + s + 1, :]
                own = jnp.sum(q * key, axis=1, keepdims=True) * inv_root
                ownb[s * KVH + k, 0:8, :] = jnp.broadcast_to(own, (8, HD))
                c0 = HQ * HD + KVH * HD + HD * k
                ownb[s * KVH + k, 8:16, :] = jnp.broadcast_to(jfull[s : s + 1, c0 : c0 + HD], (8, HD))

    def attend(s):
        if s == 0:
            loads[5].wait()
            loads[6].wait()
        inv_root = 1.0 / jnp.sqrt(F32(HD))
        pos = lax.broadcasted_iota(jnp.int32, (8, CHUNK), 1) + tp * CHUNK
        live = pos < lens[s]
        lane = lax.broadcasted_iota(jnp.int32, (8, HD), 1)
        for k in range(KVH):
            q = qf[pl.ds(8 * GROUP * k + s, 8, stride=8), :].astype(BF16)
            sc = lax.dot_general(
                q, kb[s, :, HD * k : HD * (k + 1)], NT, preferred_element_type=F32
            ) * inv_root
            sc = jnp.where(live, sc, F32(-1e30))
            m = jnp.max(sc, axis=1, keepdims=True)
            p = jnp.where(live, jnp.exp(sc - m), F32(0.0)).astype(BF16)
            l = jnp.sum(p.astype(F32), axis=1, keepdims=True)
            n = jnp.dot(p, vb[s, :, HD * k : HD * (k + 1)], preferred_element_type=F32)
            part[s * KVH + k, 0:8, :] = n
            part[s * KVH + k, 8:16, :] = jnp.where(
                lane == 0, jnp.broadcast_to(m, (8, HD)), jnp.broadcast_to(l, (8, HD))
            )

    def share():
        parts[tp] = part[pl.ds(2 * tp, 2)]
        to_peers(1, lambda t: part.at[pl.ds(2 * t, 2)], lambda: parts.at[tp])

    def combine():
        all_bytes(seven[1], small_recv.at[1])
        for n in range(2):
            own = ownb[2 * tp + n, 0:8, :]
            val = ownb[2 * tp + n, 8:16, :]
            top = own
            for t in range(8):
                top = jnp.maximum(top, jnp.broadcast_to(parts[t, n, 8:16, 0:1], (8, HD)))
            w = jnp.exp(own - top).astype(BF16).astype(F32)
            num = w * val
            den = w
            for t in range(8):
                scale = jnp.exp(jnp.broadcast_to(parts[t, n, 8:16, 0:1], (8, HD)) - top)
                num = num + parts[t, n, 0:8, :] * scale
                den = den + jnp.broadcast_to(parts[t, n, 8:16, 1:2], (8, HD)) * scale
            att[pl.ds(pl.multiple_of(16 * tp + 8 * n, 8), 8), :] = (num / den).astype(BF16).astype(F32)
        own = att.at[pl.ds(pl.multiple_of(16 * tp, 16), 16)]
        to_peers(2, lambda t: own, lambda: own)

    def finish():
        all_bytes(seven[2], small_recv.at[2])
        loads[7].wait()
        for k in range(KVH):
            for g in range(GROUP):
                h = GROUP * k + g
                amat[0:SEQ, HD * h : HD * (h + 1)] = att[pl.ds(8 * k + g, SEQ, stride=8 * KVH), :]
        decoded[...] = lax.dot_general(
            amat[0:SEQ, :].astype(BF16), wo[...], NT, preferred_element_type=F32
        ).astype(BF16)

    pieces = {"exchange": exchange, "project": project, "rotary": rotary, "share": share, "combine": combine, "finish": finish}
    for event in ORDER:
        handle(*event)
        for piece in DECODE.get(event, ()):
            if piece.startswith("attend"):
                attend(int(piece[-1]))
            else:
                pieces[piece]()
    for j in range(8):
        all_bytes(packed, twin_sem.at[j])
    all_bytes(land.at[:, pl.ds(0, QUADS * len(sent))], send_sem.at[0])
    for phase in range(3):
        all_bytes(seven[phase], small_send.at[phase])


def write_kernel(land, dec, out_q, out_o, out_d, oq, oo, sems):
    eye = jnp.where(
        lax.broadcasted_iota(jnp.int32, (256, 256), 0) == lax.broadcasted_iota(jnp.int32, (256, 256), 1), 1.0, 0.0
    ).astype(BF16)
    copies = []

    def out(src, dst, first, n):
        c = pltpu.make_async_copy(src.at[pl.ds(first, n)], dst.at[pl.ds(first, n)], sems.at[len(copies)])
        c.start()
        copies.append(c)

    d = pltpu.make_async_copy(dec, out_d, sems.at[6])
    d.start()
    for c in range(4):

        def body(i, _):
            q0 = i * 64
            w = jnp.concatenate(
                [land[2 * c + n, pl.ds(q0, 64)].reshape(256, 128) for n in range(2)], axis=1
            )
            v = lax.dot_general(eye, w, NT, preferred_element_type=F32).astype(BF16)
            at = pl.ds(pl.multiple_of(i * 256, 256), 256)
            if c < 2:
                oq[256 * c : 256 * (c + 1), at] = v
            elif c == 2:
                oq[512:576, at] = v[0:64]
                oo[384:448, at] = v[64:128]
                oo[0:128, at] = v[128:256]
            else:
                oo[128:384, at] = v
            return 0

        lax.fori_loop(0, 14, body, 0)
        if c < 2:
            out(oq, out_q, 256 * c, 256)
        elif c == 2:
            out(oq, out_q, 512, 64)
            out(oo, out_o, 384, 64)
            out(oo, out_o, 0, 128)
        else:
            out(oo, out_o, 128, 256)
    for c in copies:
        c.wait()
    d.wait()


def per_device(hidden_state, lengths, old_qkv, old_out, cache_keys, cache_values, new_qkv, new_out):
    half = ROPE_BASE ** (-2.0 * np.arange(HD // 2) / HD)
    freq = jnp.asarray(np.concatenate([half, half])[None], F32)
    any_ = pl.BlockSpec(memory_space=pl.ANY)
    hbm = pl.BlockSpec(memory_space=pltpu.HBM)
    vmem = pl.BlockSpec(memory_space=pltpu.VMEM)
    far = [
        pltpu.with_memory_space_constraint(a, pltpu.HBM)
        for a in (lengths, hidden_state, freq, old_qkv.T, old_out.T, cache_keys, cache_values, new_qkv, new_out)
    ]
    land, dec = pl.pallas_call(
        move_kernel,
        out_shape=(pltpu.VMEM((TILES, 128 * QUADS, 4, 128), BF16), pltpu.VMEM((SEQ, OC), BF16)),
        in_specs=[hbm] * 9,
        out_specs=(vmem, vmem),
        scratch_shapes=[
            pltpu.VMEM((8, TILES, QUADS, 4, 128), BF16),
            pltpu.VMEM((ROWS, 4608), BF16),
            pltpu.VMEM((ROWS, 3584), BF16),
            pltpu.VMEM((SEQ, 3584), BF16),
            pltpu.VMEM((1, HD), F32),
            pltpu.VMEM((QC, 3584), BF16),
            pltpu.VMEM((OC, 3584), BF16),
            pltpu.VMEM((SEQ, CHUNK, 512), BF16),
            pltpu.VMEM((SEQ, CHUNK, 512), BF16),
            pltpu.VMEM((16, 640), BF16),
            pltpu.VMEM((8, 16, 640), BF16),
            pltpu.VMEM((8, 4608), F32),
            pltpu.VMEM((8 * (HQ + KVH), HD), F32),
            pltpu.VMEM((PAIRS, 16, HD), F32),
            pltpu.VMEM((PAIRS, 16, HD), F32),
            pltpu.VMEM((8, 2, 16, HD), F32),
            pltpu.VMEM((PAIRS * 8, HD), F32),
            pltpu.VMEM((8, 3584), F32),
            pltpu.SMEM((SEQ,), jnp.int32),
            pltpu.SemaphoreType.DMA((9,)),
            pltpu.SemaphoreType.DMA((64,)),
            pltpu.SemaphoreType.DMA((8,)),
            pltpu.SemaphoreType.DMA((1,)),
            pltpu.SemaphoreType.DMA((3,)),
            pltpu.SemaphoreType.DMA((3,)),
        ],
        compiler_params=pltpu.CompilerParams(
            collective_id=0, has_side_effects=True, vmem_limit_bytes=40 * 1024 * 1024
        ),
        name="move",
    )(*far)
    qkv_tp, out_tp, decoded = pl.pallas_call(
        write_kernel,
        out_shape=(pltpu.HBM((QC, 3584), BF16), pltpu.HBM((OC, 3584), BF16), pltpu.HBM((SEQ, OC), BF16)),
        in_specs=[vmem, vmem],
        out_specs=(hbm, hbm, hbm),
        scratch_shapes=[
            pltpu.VMEM((QC, 3584), BF16),
            pltpu.VMEM((OC, 3584), BF16),
            pltpu.SemaphoreType.DMA((7,)),
        ],
        compiler_params=pltpu.CompilerParams(vmem_limit_bytes=24 * 1024 * 1024),
        name="write",
    )(land, dec)
    return decoded, qkv_tp.T, out_tp.T


def solution(mesh):
    in_specs = (
        P("rep", None),
        P("rep"),
        P(None, "tp"),
        P(None, "tp"),
        P("rep", "tp", None),
        P("rep", "tp", None),
        P(("rep", "tp"), None),
        P(("rep", "tp"), None),
    )
    out_specs = (P("rep", "tp"), P(None, "tp"), P(None, "tp"))
    return jax.shard_map(per_device, mesh=mesh, in_specs=in_specs, out_specs=out_specs, check_vma=False)
```

```python
import jax
import jax.numpy as jnp
import numpy as np
from jax import lax
from jax.experimental import pallas as pl
from jax.experimental.pallas import tpu as pltpu
from jax.sharding import PartitionSpec as P

HQ = 28
KVH = 4
HD = 128
GROUP = HQ // KVH
ROPE_BASE = 1000000.0
ROWS = 28
QC = 576
OC = 448
TILES = 8
QUADS = ROWS // 4
SEQ = 4
WIDE = 896
CHUNK = 512
PAIRS = SEQ * KVH

ITEMS = ((0, 0), (0, 1), (1, 0), (3, 0), (1, 1), (3, 1), (2, 0), (2, 1))
X_FIRST = (False, True, True, True, True, False, False, False)
ORDER = (
    ("O", 0), ("O", 1), ("P", 0), ("D", 0), ("U", 0), ("O", 2), ("O", 3), ("O", 4), ("O", 5), ("P", 1), ("D", 1),
    ("U", 1), ("O", 6), ("d", 0), ("V", 0), ("U", 2), ("O", 7), ("u", 0), ("D", 2), ("U", 3), ("P", 2), ("D", 3),
    ("U", 4), ("P", 3), ("D", 4), ("U", 5), ("P", 4), ("D", 5), ("V", 1), ("P", 5), ("d", 1), ("u", 1), ("P", 6),
    ("D", 6), ("U", 6), ("v", 0), ("D", 7), ("U", 7), ("P", 7), ("V", 2), ("V", 3), ("d", 2), ("u", 2), ("u", 5),
    ("d", 5), ("V", 4), ("V", 5), ("d", 3), ("d", 6), ("u", 3), ("d", 4), ("u", 4), ("u", 6), ("d", 7), ("v", 1),
    ("V", 7), ("v", 2), ("u", 7), ("V", 6), ("v", 3), ("v", 4), ("v", 5), ("v", 7), ("v", 6),
)
DECODE = {
    ("O", 0): ("exchange", "project"), ("U", 1): ("rotary",), ("U", 2): ("attend0",), ("U", 4): ("attend1",),
    ("P", 4): ("attend2",), ("P", 6): ("attend3", "share"), ("V", 5): ("combine",), ("d", 7): ("finish",),
}
F32 = jnp.float32
BF16 = jnp.bfloat16
NT = (((1,), (1,)), ((), ()))


def move_kernel(
    lengths, hidden, freq, old_qkv, old_out, keys, values, new_qkv, new_out,
    land, decoded,
    packed, nq, no, hid, frq, wq, wo, kb, vb,
    jown, jall, jfull, qf, ownb, part, parts, att, amat,
    lens, load_sem, recv_sem, twin_sem, send_sem, small_recv, small_send,
):
    rep = lax.axis_index("rep")
    tp = lax.axis_index("tp")
    core = rep % 2
    x_lo = (rep // 2) % 2
    z = rep // 4
    y = tp // 2
    x_hi = tp % 2
    z_up = (z + 1) % 4
    z_dn = (z + 3) % 4
    z_op = (z + 2) % 4
    x_ot = 1 - x_lo

    def rep_of(zz, xx, cc):
        return (zz * 2 + xx) * 2 + cc

    loads = []
    for n, (src, dst) in enumerate(
        ((new_qkv, nq), (new_out, no), (hidden, hid), (freq, frq), (old_qkv, wq), (keys, kb), (values, vb), (old_out, wo), (lengths, lens))
    ):
        c = pltpu.make_async_copy(src, dst, load_sem.at[n])
        c.start()
        loads.append(c)

    barrier = pltpu.get_barrier_semaphore()
    friends = []
    for dy in range(4):
        for f in range(2):
            t = ((y + dy) % 4) * 2 + (x_hi + f) % 2
            if (dy, f) != (0, 0):
                friends.append((rep, t))
            if f == 1:
                friends.append((rep_of(z, x_ot, core), t))
    friends.append((rep_of(z, x_ot, core), tp))
    friends.append((rep_of(z_up, x_lo, core), tp))
    friends.append((rep_of(z_dn, x_lo, core), tp))
    friends.append((rep_of(z, x_lo, 1 - core), tp))
    for r, t in friends:
        pl.semaphore_signal(barrier, inc=1, device_id={"rep": r, "tp": t}, device_id_type=pl.DeviceIdType.MESH)

    loads[0].wait()
    loads[1].wait()
    for t in range(8):
        a = nq[:, QC * t : QC * (t + 1)]
        b = no[:, OC * t : OC * (t + 1)]
        for k in range(TILES):
            if k < 4:
                v = a[:, 128 * k : 128 * (k + 1)]
            elif k == 4:
                v = jnp.concatenate([a[:, 512:576], b[:, 384:448]], axis=1)
            else:
                v = b[:, 128 * (k - 5) : 128 * (k - 4)]
            packed[t, k] = v.reshape(QUADS, 4, 128)
    mine = rep * 8 + tp
    land[:, pl.ds(QUADS * mine, QUADS)] = packed[tp]
    pl.semaphore_wait(barrier, len(friends))

    sent = []

    def slot_key(slot):
        return slot // 16 * 8 + slot % 8

    def place(slot):
        return land.at[:, pl.ds(QUADS * slot, QUADS)]

    def put(src, slot, r, t, sem=None):
        c = pltpu.make_async_remote_copy(
            src_ref=src, dst_ref=place(slot), send_sem=send_sem.at[0],
            recv_sem=recv_sem.at[slot_key(slot)] if sem is None else sem,
            device_id={"rep": r, "tp": t}, device_id_type=pl.DeviceIdType.MESH,
        )
        c.start()
        sent.append(c)

    def arrived(slot):
        pltpu.make_async_remote_copy(
            src_ref=place(slot), dst_ref=place(slot), send_sem=send_sem.at[0],
            recv_sem=recv_sem.at[slot_key(slot)],
            device_id={"rep": rep, "tp": tp}, device_id_type=pl.DeviceIdType.MESH,
        ).wait_recv()

    def slot_of(zz, xx, item):
        dy, f = item
        r = rep_of(zz, (xx + f) % 2, core)
        t = ((y + dy) % 4) * 2 + (x_hi + f) % 2
        return r * 8 + t

    def exchange():
        for dy, f in ITEMS[1:]:
            t = ((y + 4 - dy) % 4) * 2 + (x_hi + f) % 2
            put(packed.at[t], mine, rep_of(z, (x_lo + f) % 2, core), t)

    def up(slot):
        put(place(slot), slot, rep_of(z_up, x_lo, core), tp)

    def down(slot):
        put(place(slot), slot, rep_of(z_dn, x_lo, core), tp)

    def across(slot):
        put(place(slot), slot, rep_of(z, x_ot, core), tp)

    def twin(slot, j):
        put(place(slot), slot, rep_of(z, x_lo, 1 - core), tp, twin_sem.at[j])

    def handle(kind, j):
        first, fwd_up = X_FIRST[j], j % 2 == 0
        zz = {"o": z, "p": z, "d": z_dn, "u": z_up, "v": z_op}[kind.lower()]
        xx = x_lo if kind in "ODUV" else x_ot
        b = slot_of(zz, xx, ITEMS[j])
        if (kind, j) != ("O", 0):
            arrived(b)
        if kind == "O" or (kind == "P" and first):
            up(b)
            down(b)
        if (kind == "D" and fwd_up) or (kind == "d" and first and not fwd_up):
            up(b)
        if (kind == "U" and not fwd_up) or (kind == "u" and first and fwd_up):
            down(b)
        if kind == "O" or (kind in "DUV" and not first):
            across(b)
        twin(b, j)

    small = []

    def to_peers(phase, src_of, dst_of):
        for n in range(1, 8):
            t = (tp + n) % 8
            c = pltpu.make_async_remote_copy(
                src_ref=src_of(t), dst_ref=dst_of(), send_sem=small_send.at[phase],
                recv_sem=small_recv.at[phase],
                device_id={"rep": rep, "tp": t}, device_id_type=pl.DeviceIdType.MESH,
            )
            c.start()
            small.append(c)

    def all_bytes(ref, sem):
        pltpu.make_async_copy(ref, ref, sem).wait()

    seven = (jall.at[pl.ds(0, 7)], parts.at[pl.ds(0, 7)], att.at[pl.ds(0, 7 * 16)])

    def project():
        loads[2].wait()
        loads[4].wait()
        res = lax.dot_general(hid[...], wq[...], NT, preferred_element_type=F32).astype(BF16)
        jown[0:SEQ, 0:QC] = res
        jall[tp, 0:SEQ, 0:QC] = res
        to_peers(0, lambda t: jown, lambda: jall.at[tp])

    def rotary():
        all_bytes(seven[0], small_recv.at[0])
        loads[3].wait()
        loads[8].wait()
        row = lax.broadcasted_iota(jnp.int32, (8, HD), 0)
        lane = lax.broadcasted_iota(jnp.int32, (8, HD), 1)
        pos = jnp.zeros((8, HD), F32)
        for s in range(SEQ):
            pos = jnp.where(row == s, lens[s].astype(F32), pos)
        angles = pos * jnp.broadcast_to(frq[0:1, :], (8, HD))
        cos2 = jnp.cos(angles)[0:SEQ]
        sin2 = jnp.where(lane < HD // 2, -jnp.sin(angles), jnp.sin(angles))[0:SEQ]
        for t in range(8):
            jfull[0:SEQ, QC * t : QC * (t + 1)] = jall[t, 0:SEQ, 0:QC].astype(F32)
        for h in range(HQ + KVH):
            x = jfull[0:SEQ, HD * h : HD * (h + 1)]
            r = x * cos2 + pltpu.roll(x, HD // 2, 1) * sin2
            qf[8 * h : 8 * h + SEQ, :] = r.astype(BF16).astype(F32)
        inv_root = 1.0 / jnp.sqrt(F32(HD))
        for s in range(SEQ):
            for k in range(KVH):
                q = qf[pl.ds(8 * GROUP * k + s, 8, stride=8), :]
                key = qf[8 * (HQ + k) + s : 8 * (HQ + k) + s + 1, :]
                own = jnp.sum(q * key, axis=1, keepdims=True) * inv_root
                ownb[s * KVH + k, 0:8, :] = jnp.broadcast_to(own, (8, HD))
                c0 = HQ * HD + KVH * HD + HD * k
                ownb[s * KVH + k, 8:16, :] = jnp.broadcast_to(jfull[s : s + 1, c0 : c0 + HD], (8, HD))

    def attend(s):
        if s == 0:
            loads[5].wait()
            loads[6].wait()
        inv_root = 1.0 / jnp.sqrt(F32(HD))
        pos = lax.broadcasted_iota(jnp.int32, (8, CHUNK), 1) + tp * CHUNK
        live = pos < lens[s]
        lane = lax.broadcasted_iota(jnp.int32, (8, HD), 1)
        for k in range(KVH):
            q = qf[pl.ds(8 * GROUP * k + s, 8, stride=8), :].astype(BF16)
            sc = lax.dot_general(
                q, kb[s, :, HD * k : HD * (k + 1)], NT, preferred_element_type=F32
            ) * inv_root
            sc = jnp.where(live, sc, F32(-1e30))
            m = jnp.max(sc, axis=1, keepdims=True)
            p = jnp.where(live, jnp.exp(sc - m), F32(0.0)).astype(BF16)
            l = jnp.sum(p.astype(F32), axis=1, keepdims=True)
            n = jnp.dot(p, vb[s, :, HD * k : HD * (k + 1)], preferred_element_type=F32)
            part[s * KVH + k, 0:8, :] = n
            part[s * KVH + k, 8:16, :] = jnp.where(
                lane == 0, jnp.broadcast_to(m, (8, HD)), jnp.broadcast_to(l, (8, HD))
            )

    def share():
        parts[tp] = part[pl.ds(2 * tp, 2)]
        to_peers(1, lambda t: part.at[pl.ds(2 * t, 2)], lambda: parts.at[tp])

    def combine():
        all_bytes(seven[1], small_recv.at[1])
        for n in range(2):
            own = ownb[2 * tp + n, 0:8, :]
            val = ownb[2 * tp + n, 8:16, :]
            top = own
            for t in range(8):
                top = jnp.maximum(top, jnp.broadcast_to(parts[t, n, 8:16, 0:1], (8, HD)))
            w = jnp.exp(own - top).astype(BF16).astype(F32)
            num = w * val
            den = w
            for t in range(8):
                scale = jnp.exp(jnp.broadcast_to(parts[t, n, 8:16, 0:1], (8, HD)) - top)
                num = num + parts[t, n, 0:8, :] * scale
                den = den + jnp.broadcast_to(parts[t, n, 8:16, 1:2], (8, HD)) * scale
            att[pl.ds(pl.multiple_of(16 * tp + 8 * n, 8), 8), :] = (num / den).astype(BF16).astype(F32)
        own = att.at[pl.ds(pl.multiple_of(16 * tp, 16), 16)]
        to_peers(2, lambda t: own, lambda: own)

    def finish():
        all_bytes(seven[2], small_recv.at[2])
        loads[7].wait()
        for k in range(KVH):
            for g in range(GROUP):
                h = GROUP * k + g
                amat[0:SEQ, HD * h : HD * (h + 1)] = att[pl.ds(8 * k + g, SEQ, stride=8 * KVH), :]
        decoded[...] = lax.dot_general(
            amat[0:SEQ, :].astype(BF16), wo[...], NT, preferred_element_type=F32
        ).astype(BF16)

    pieces = {"exchange": exchange, "project": project, "rotary": rotary, "share": share, "combine": combine, "finish": finish}
    for event in ORDER:
        handle(*event)
        for piece in DECODE.get(event, ()):
            if piece.startswith("attend"):
                attend(int(piece[-1]))
            else:
                pieces[piece]()
    for j in range(8):
        all_bytes(packed, twin_sem.at[j])
    all_bytes(land.at[:, pl.ds(0, QUADS * len(sent))], send_sem.at[0])
    for phase in range(3):
        all_bytes(seven[phase], small_send.at[phase])


def write_kernel(land, dec, out_q, out_o, out_d, oq, oo, sems):
    copies = []

    def out(src, dst, first, n):
        c = pltpu.make_async_copy(src.at[pl.ds(first, n)], dst.at[pl.ds(first, n)], sems.at[len(copies)])
        c.start()
        copies.append(c)

    d = pltpu.make_async_copy(dec, out_d, sems.at[9])
    d.start()
    for k in range(TILES):

        def body(i, _):
            v = land[k, pl.ds(i * (WIDE // 4), WIDE // 4)].reshape(WIDE, 128).T
            at = pl.ds(pl.multiple_of(i * WIDE, WIDE), WIDE)
            if k < 4:
                oq[128 * k : 128 * (k + 1), at] = v
            elif k == 4:
                oq[512:576, at] = v[0:64]
                oo[384:448, at] = v[64:128]
            else:
                oo[128 * (k - 5) : 128 * (k - 4), at] = v
            return 0

        lax.fori_loop(0, 3584 // WIDE, body, 0)
        if k < 4:
            out(oq, out_q, 128 * k, 128)
        elif k == 4:
            out(oq, out_q, 512, 64)
            out(oo, out_o, 384, 64)
        else:
            out(oo, out_o, 128 * (k - 5), 128)
    for c in copies:
        c.wait()
    d.wait()


def per_device(hidden_state, lengths, old_qkv, old_out, cache_keys, cache_values, new_qkv, new_out):
    half = ROPE_BASE ** (-2.0 * np.arange(HD // 2) / HD)
    freq = jnp.asarray(np.concatenate([half, half])[None], F32)
    any_ = pl.BlockSpec(memory_space=pl.ANY)
    hbm = pl.BlockSpec(memory_space=pltpu.HBM)
    vmem = pl.BlockSpec(memory_space=pltpu.VMEM)
    far = [
        pltpu.with_memory_space_constraint(a, pltpu.HBM)
        for a in (lengths, hidden_state, freq, old_qkv.T, old_out.T, cache_keys, cache_values, new_qkv, new_out)
    ]
    land, dec = pl.pallas_call(
        move_kernel,
        out_shape=(pltpu.VMEM((TILES, 128 * QUADS, 4, 128), BF16), pltpu.VMEM((SEQ, OC), BF16)),
        in_specs=[hbm] * 9,
        out_specs=(vmem, vmem),
        scratch_shapes=[
            pltpu.VMEM((8, TILES, QUADS, 4, 128), BF16),
            pltpu.VMEM((ROWS, 4608), BF16),
            pltpu.VMEM((ROWS, 3584), BF16),
            pltpu.VMEM((SEQ, 3584), BF16),
            pltpu.VMEM((1, HD), F32),
            pltpu.VMEM((QC, 3584), BF16),
            pltpu.VMEM((OC, 3584), BF16),
            pltpu.VMEM((SEQ, CHUNK, 512), BF16),
            pltpu.VMEM((SEQ, CHUNK, 512), BF16),
            pltpu.VMEM((16, 640), BF16),
            pltpu.VMEM((8, 16, 640), BF16),
            pltpu.VMEM((8, 4608), F32),
            pltpu.VMEM((8 * (HQ + KVH), HD), F32),
            pltpu.VMEM((PAIRS, 16, HD), F32),
            pltpu.VMEM((PAIRS, 16, HD), F32),
            pltpu.VMEM((8, 2, 16, HD), F32),
            pltpu.VMEM((PAIRS * 8, HD), F32),
            pltpu.VMEM((8, 3584), F32),
            pltpu.SMEM((SEQ,), jnp.int32),
            pltpu.SemaphoreType.DMA((9,)),
            pltpu.SemaphoreType.DMA((64,)),
            pltpu.SemaphoreType.DMA((8,)),
            pltpu.SemaphoreType.DMA((1,)),
            pltpu.SemaphoreType.DMA((3,)),
            pltpu.SemaphoreType.DMA((3,)),
        ],
        compiler_params=pltpu.CompilerParams(
            collective_id=0, has_side_effects=True, vmem_limit_bytes=40 * 1024 * 1024
        ),
        name="move",
    )(*far)
    qkv_tp, out_tp, decoded = pl.pallas_call(
        write_kernel,
        out_shape=(pltpu.HBM((QC, 3584), BF16), pltpu.HBM((OC, 3584), BF16), pltpu.HBM((SEQ, OC), BF16)),
        in_specs=[vmem, vmem],
        out_specs=(hbm, hbm, hbm),
        scratch_shapes=[
            pltpu.VMEM((QC, 3584), BF16),
            pltpu.VMEM((OC, 3584), BF16),
            pltpu.SemaphoreType.DMA((10,)),
        ],
        compiler_params=pltpu.CompilerParams(vmem_limit_bytes=24 * 1024 * 1024),
        name="write",
    )(land, dec)
    return decoded, qkv_tp.T, out_tp.T


def solution(mesh):
    in_specs = (
        P("rep", None),
        P("rep"),
        P(None, "tp"),
        P(None, "tp"),
        P("rep", "tp", None),
        P("rep", "tp", None),
        P(("rep", "tp"), None),
        P(("rep", "tp"), None),
    )
    out_specs = (P("rep", "tp"), P(None, "tp"), P(None, "tp"))
    return jax.shard_map(per_device, mesh=mesh, in_specs=in_specs, out_specs=out_specs, check_vma=False)
```

```python
import jax
import jax.numpy as jnp
import numpy as np
from jax import lax
from jax.experimental import pallas as pl
from jax.experimental.pallas import tpu as pltpu
from jax.sharding import PartitionSpec as P

HQ = 28
KVH = 4
HD = 128
GROUP = HQ // KVH
ROPE_BASE = 1000000.0
ROWS = 28
QC = 576
OC = 448
TILES = 8
QUADS = ROWS // 4
SEQ = 4
CHUNK = 512
PAIRS = SEQ * KVH

ITEMS = ((0, 0), (0, 1), (1, 0), (3, 0), (1, 1), (3, 1), (2, 0), (2, 1))
X_FIRST = (False, False, True, True, True, True, True, False)
PASS_UP = (True, False, True, False, True, False, True, True)
ORDER = (
    ("O", 0), ("O", 1), ("P", 0), ("D", 0), ("U", 0), ("O", 2), ("O", 3), ("O", 4), ("O", 5), ("P", 1), ("D", 1),
    ("U", 1), ("O", 6), ("d", 0), ("V", 0), ("U", 2), ("O", 7), ("u", 0), ("D", 2), ("U", 3), ("P", 2), ("D", 3),
    ("U", 4), ("P", 3), ("D", 4), ("U", 5), ("P", 4), ("D", 5), ("V", 1), ("P", 5), ("D", 6), ("U", 6), ("d", 1),
    ("D", 7), ("U", 7), ("u", 1), ("V", 2), ("V", 3), ("P", 6), ("d", 2), ("u", 2), ("v", 0), ("V", 4), ("V", 5),
    ("P", 7), ("d", 3), ("u", 3), ("d", 4), ("u", 4), ("v", 1), ("u", 5), ("V", 6), ("d", 7), ("d", 5), ("v", 2),
    ("u", 7), ("u", 6), ("V", 7), ("d", 6), ("v", 4), ("v", 3), ("v", 6), ("v", 7), ("v", 5),
)
DECODE = {
    ("O", 0): ("exchange", "project"), ("U", 1): ("rotary", "attend0"), ("V", 0): ("attend1",), ("U", 2): ("attend2",),
    ("O", 7): ("attend3", "share"), ("P", 6): ("combine",), ("V", 7): ("finish",),
}
F32 = jnp.float32
BF16 = jnp.bfloat16
NT = (((1,), (1,)), ((), ()))


def move_kernel(
    lengths, hidden, freq, old_qkv, old_out, keys, values, new_qkv, new_out,
    land, decoded,
    packed, nq, no, hid, frq, wq, wo, kb, vb,
    jown, jall, jfull, qf, ownb, part, parts, att, attf, amat,
    lens, load_sem, recv_sem, twin_sem, send_sem, small_recv, small_send,
):
    rep = lax.axis_index("rep")
    tp = lax.axis_index("tp")
    core = rep % 2
    x_lo = (rep // 2) % 2
    z = rep // 4
    y = tp // 2
    x_hi = tp % 2
    z_up = (z + 1) % 4
    z_dn = (z + 3) % 4
    z_op = (z + 2) % 4
    x_ot = 1 - x_lo

    def rep_of(zz, xx, cc):
        return (zz * 2 + xx) * 2 + cc

    loads = []
    for n, (src, dst) in enumerate(
        ((new_qkv, nq), (new_out, no), (hidden, hid), (freq, frq), (old_qkv, wq), (keys, kb), (values, vb), (old_out, wo), (lengths, lens))
    ):
        c = pltpu.make_async_copy(src, dst, load_sem.at[n])
        c.start()
        loads.append(c)

    barrier = pltpu.get_barrier_semaphore()
    friends = []
    for dy in range(4):
        for f in range(2):
            t = ((y + dy) % 4) * 2 + (x_hi + f) % 2
            if (dy, f) != (0, 0):
                friends.append((rep, t))
            if f == 1:
                friends.append((rep_of(z, x_ot, core), t))
    friends.append((rep_of(z, x_ot, core), tp))
    friends.append((rep_of(z_up, x_lo, core), tp))
    friends.append((rep_of(z_dn, x_lo, core), tp))
    friends.append((rep_of(z, x_lo, 1 - core), tp))
    for r, t in friends:
        pl.semaphore_signal(barrier, inc=1, device_id={"rep": r, "tp": t}, device_id_type=pl.DeviceIdType.MESH)

    loads[0].wait()
    loads[1].wait()
    for t in range(8):
        a = nq[:, QC * t : QC * (t + 1)]
        b = no[:, OC * t : OC * (t + 1)]
        for k in range(TILES):
            if k < 4:
                v = a[:, 128 * k : 128 * (k + 1)]
            elif k == 4:
                v = jnp.concatenate([a[:, 512:576], b[:, 384:448]], axis=1)
            else:
                v = b[:, 128 * (k - 5) : 128 * (k - 4)]
            packed[t, k] = v.reshape(QUADS, 4, 128)
    mine = rep * 8 + tp
    land[:, pl.ds(QUADS * mine, QUADS)] = packed[tp]
    pl.semaphore_wait(barrier, len(friends))

    sent = []

    def slot_key(slot):
        return slot // 16 * 8 + slot % 8

    def place(slot):
        return land.at[:, pl.ds(QUADS * slot, QUADS)]

    def put(src, slot, r, t, sem=None):
        c = pltpu.make_async_remote_copy(
            src_ref=src, dst_ref=place(slot), send_sem=send_sem.at[0],
            recv_sem=recv_sem.at[slot_key(slot)] if sem is None else sem,
            device_id={"rep": r, "tp": t}, device_id_type=pl.DeviceIdType.MESH,
        )
        c.start()
        sent.append(c)

    def arrived(slot):
        pltpu.make_async_remote_copy(
            src_ref=place(slot), dst_ref=place(slot), send_sem=send_sem.at[0],
            recv_sem=recv_sem.at[slot_key(slot)],
            device_id={"rep": rep, "tp": tp}, device_id_type=pl.DeviceIdType.MESH,
        ).wait_recv()

    def slot_of(zz, xx, item):
        dy, f = item
        r = rep_of(zz, (xx + f) % 2, core)
        t = ((y + dy) % 4) * 2 + (x_hi + f) % 2
        return r * 8 + t

    def exchange():
        for dy, f in ITEMS[1:]:
            t = ((y + 4 - dy) % 4) * 2 + (x_hi + f) % 2
            put(packed.at[t], mine, rep_of(z, (x_lo + f) % 2, core), t)

    def up(slot):
        put(place(slot), slot, rep_of(z_up, x_lo, core), tp)

    def down(slot):
        put(place(slot), slot, rep_of(z_dn, x_lo, core), tp)

    def across(slot):
        put(place(slot), slot, rep_of(z, x_ot, core), tp)

    def twin(slot, j):
        put(place(slot), slot, rep_of(z, x_lo, 1 - core), tp, twin_sem.at[j])

    def handle(kind, j):
        first, fwd_up = X_FIRST[j], PASS_UP[j]
        zz = {"o": z, "p": z, "d": z_dn, "u": z_up, "v": z_op}[kind.lower()]
        xx = x_lo if kind in "ODUV" else x_ot
        b = slot_of(zz, xx, ITEMS[j])
        if (kind, j) != ("O", 0):
            arrived(b)
        if kind == "O" or (kind == "P" and first):
            up(b)
            down(b)
        if (kind == "D" and fwd_up) or (kind == "d" and first and not fwd_up):
            up(b)
        if (kind == "U" and not fwd_up) or (kind == "u" and first and fwd_up):
            down(b)
        if kind == "O" or (kind in "DUV" and not first):
            across(b)
        twin(b, j)

    small = []

    def to_peers(phase, src_of, dst_of):
        for n in range(1, 8):
            t = (tp + n) % 8
            c = pltpu.make_async_remote_copy(
                src_ref=src_of(t), dst_ref=dst_of(), send_sem=small_send.at[phase],
                recv_sem=small_recv.at[phase],
                device_id={"rep": rep, "tp": t}, device_id_type=pl.DeviceIdType.MESH,
            )
            c.start()
            small.append(c)

    def all_bytes(ref, sem):
        pltpu.make_async_copy(ref, ref, sem).wait()

    seven = (jall.at[pl.ds(0, 7)], parts.at[pl.ds(0, 7)], att.at[pl.ds(0, 7 * 16)])

    def project():
        loads[2].wait()
        loads[4].wait()
        res = lax.dot_general(hid[...], wq[...], NT, preferred_element_type=F32).astype(BF16)
        jown[:, 0:QC] = res
        jall[tp, :, 0:QC] = res
        to_peers(0, lambda t: jown, lambda: jall.at[tp])

    def rotary():
        all_bytes(seven[0], small_recv.at[0])
        loads[3].wait()
        loads[8].wait()
        row = lax.broadcasted_iota(jnp.int32, (8, HD), 0)
        lane = lax.broadcasted_iota(jnp.int32, (8, HD), 1)
        pos = jnp.zeros((8, HD), F32)
        for s in range(SEQ):
            pos = jnp.where(row == s, lens[s].astype(F32), pos)
        angles = pos * jnp.broadcast_to(frq[0:1, :], (8, HD))
        cos2 = jnp.cos(angles)[0:SEQ]
        sin2 = jnp.where(lane < HD // 2, -jnp.sin(angles), jnp.sin(angles))[0:SEQ]
        for t in range(8):
            jfull[0:SEQ, QC * t : QC * (t + 1)] = jall[t, :, 0:QC].astype(F32)
        for h in range(HQ + KVH):
            x = jfull[0:SEQ, HD * h : HD * (h + 1)]
            r = x * cos2 + pltpu.roll(x, HD // 2, 1) * sin2
            qf[8 * h : 8 * h + SEQ, :] = r.astype(BF16).astype(F32)
        inv_root = 1.0 / jnp.sqrt(F32(HD))
        for s in range(SEQ):
            for k in range(KVH):
                q = qf[pl.ds(8 * GROUP * k + s, 8, stride=8), :]
                key = qf[8 * (HQ + k) + s : 8 * (HQ + k) + s + 1, :]
                own = jnp.sum(q * key, axis=1, keepdims=True) * inv_root
                ownb[s * KVH + k, 0:8, :] = jnp.broadcast_to(own, (8, HD))
                c0 = HQ * HD + KVH * HD + HD * k
                ownb[s * KVH + k, 8:16, :] = jnp.broadcast_to(jfull[s : s + 1, c0 : c0 + HD], (8, HD))

    def attend(s):
        if s == 0:
            loads[5].wait()
            loads[6].wait()
        inv_root = 1.0 / jnp.sqrt(F32(HD))
        pos = lax.broadcasted_iota(jnp.int32, (8, CHUNK), 1) + tp * CHUNK
        live = pos < lens[s]
        row = lax.broadcasted_iota(jnp.int32, (8, HD), 0)
        lane = lax.broadcasted_iota(jnp.int32, (8, HD), 1)
        for k in range(KVH):
            q = qf[pl.ds(8 * GROUP * k + s, 8, stride=8), :].astype(BF16)
            sc = lax.dot_general(
                q, kb[s, :, HD * k : HD * (k + 1)], NT, preferred_element_type=F32
            ) * inv_root
            sc = jnp.where(live, sc, F32(-1e30))
            m = jnp.max(sc, axis=1, keepdims=True)
            p = jnp.where(live, jnp.exp(sc - m), F32(0.0)).astype(BF16)
            l = jnp.sum(p.astype(F32), axis=1, keepdims=True)
            n = jnp.dot(p, vb[s, :, HD * k : HD * (k + 1)], preferred_element_type=F32)
            stats = jnp.sum(
                jnp.where(lane == row, jnp.broadcast_to(m, (8, HD)), 0.0)
                + jnp.where(lane == row + 8, jnp.broadcast_to(l, (8, HD)), 0.0),
                axis=0,
                keepdims=True,
            )
            part[s * KVH + k] = jnp.where(row < GROUP, n, jnp.broadcast_to(stats, (8, HD)))

    def share():
        parts[tp] = part[pl.ds(2 * tp, 2)]
        to_peers(1, lambda t: part.at[pl.ds(2 * t, 2)], lambda: parts.at[tp])

    def combine():
        all_bytes(seven[1], small_recv.at[1])
        row = lax.broadcasted_iota(jnp.int32, (8, HD), 0)
        lane = lax.broadcasted_iota(jnp.int32, (8, HD), 1)
        done = []
        for n in range(2):
            own = ownb[2 * tp + n, 0:8, :]
            val = ownb[2 * tp + n, 8:16, :]
            maxima, totals = [], []
            top = own
            for t in range(8):
                stats = jnp.broadcast_to(parts[t, n, GROUP : GROUP + 1, :], (8, HD))
                m = jnp.sum(jnp.where(lane == row, stats, 0.0), axis=1, keepdims=True)
                l = jnp.sum(jnp.where(lane == row + 8, stats, 0.0), axis=1, keepdims=True)
                maxima.append(jnp.broadcast_to(m, (8, HD)))
                totals.append(jnp.broadcast_to(l, (8, HD)))
                top = jnp.maximum(top, maxima[t])
            w = jnp.exp(own - top).astype(BF16).astype(F32)
            num = w * val
            den = w
            for t in range(8):
                scale = jnp.exp(maxima[t] - top)
                num = num + parts[t, n] * scale
                den = den + totals[t] * scale
            done.append(num / den)
        att[pl.ds(pl.multiple_of(16 * tp, 16), 16), :] = jnp.concatenate(done, axis=0).astype(BF16)
        own = att.at[pl.ds(pl.multiple_of(16 * tp, 16), 16)]
        to_peers(2, lambda t: own, lambda: own)

    def finish():
        all_bytes(seven[2], small_recv.at[2])
        loads[7].wait()
        attf[...] = att[...].astype(F32)
        for k in range(KVH):
            for g in range(GROUP):
                h = GROUP * k + g
                amat[0:SEQ, HD * h : HD * (h + 1)] = attf[pl.ds(8 * k + g, SEQ, stride=8 * KVH), :]
        decoded[...] = lax.dot_general(
            amat[0:SEQ, :].astype(BF16), wo[...], NT, preferred_element_type=F32
        ).astype(BF16)

    pieces = {"exchange": exchange, "project": project, "rotary": rotary, "share": share, "combine": combine, "finish": finish}
    for event in ORDER:
        handle(*event)
        for piece in DECODE.get(event, ()):
            if piece.startswith("attend"):
                attend(int(piece[-1]))
            else:
                pieces[piece]()
    for j in range(8):
        all_bytes(packed, twin_sem.at[j])
    all_bytes(land.at[:, pl.ds(0, QUADS * len(sent))], send_sem.at[0])
    for phase in range(3):
        all_bytes(seven[phase], small_send.at[phase])


def write_kernel(land, dec, out_q, out_o, out_d, oq, oo, sems):
    copies = []

    def out(src, dst, first, n):
        c = pltpu.make_async_copy(src.at[pl.ds(first, n)], dst.at[pl.ds(first, n)], sems.at[len(copies)])
        c.start()
        copies.append(c)

    d = pltpu.make_async_copy(dec, out_d, sems.at[9])
    d.start()
    for k in range(TILES):
        v = land[k].T
        if k < 4:
            oq[128 * k : 128 * (k + 1)] = v
        elif k == 4:
            oq[512:576] = v[0:64]
            oo[384:448] = v[64:128]
        else:
            oo[128 * (k - 5) : 128 * (k - 4)] = v
        if k < 4:
            out(oq, out_q, 128 * k, 128)
        elif k == 4:
            out(oq, out_q, 512, 64)
            out(oo, out_o, 384, 64)
        else:
            out(oo, out_o, 128 * (k - 5), 128)
    for c in copies:
        c.wait()
    d.wait()


def per_device(hidden_state, lengths, old_qkv, old_out, cache_keys, cache_values, new_qkv, new_out):
    half = ROPE_BASE ** (-2.0 * np.arange(HD // 2) / HD)
    freq = jnp.asarray(np.concatenate([half, half])[None], F32)
    any_ = pl.BlockSpec(memory_space=pl.ANY)
    hbm = pl.BlockSpec(memory_space=pltpu.HBM)
    vmem = pl.BlockSpec(memory_space=pltpu.VMEM)
    far = [
        pltpu.with_memory_space_constraint(a, pltpu.HBM)
        for a in (lengths, hidden_state, freq, old_qkv.T, old_out.T, cache_keys, cache_values, new_qkv, new_out)
    ]
    land, dec = pl.pallas_call(
        move_kernel,
        out_shape=(pltpu.VMEM((TILES, 128 * QUADS, 4, 128), BF16), pltpu.VMEM((SEQ, OC), BF16)),
        in_specs=[hbm] * 9,
        out_specs=(vmem, vmem),
        scratch_shapes=[
            pltpu.VMEM((8, TILES, QUADS, 4, 128), BF16),
            pltpu.VMEM((ROWS, 4608), BF16),
            pltpu.VMEM((ROWS, 3584), BF16),
            pltpu.VMEM((SEQ, 3584), BF16),
            pltpu.VMEM((1, HD), F32),
            pltpu.VMEM((QC, 3584), BF16),
            pltpu.VMEM((OC, 3584), BF16),
            pltpu.VMEM((SEQ, CHUNK, 512), BF16),
            pltpu.VMEM((SEQ, CHUNK, 512), BF16),
            pltpu.VMEM((SEQ, 640), BF16),
            pltpu.VMEM((8, SEQ, 640), BF16),
            pltpu.VMEM((8, 4608), F32),
            pltpu.VMEM((8 * (HQ + KVH), HD), F32),
            pltpu.VMEM((PAIRS, 16, HD), F32),
            pltpu.VMEM((PAIRS, 8, HD), F32),
            pltpu.VMEM((8, 2, 8, HD), F32),
            pltpu.VMEM((PAIRS * 8, HD), BF16),
            pltpu.VMEM((PAIRS * 8, HD), F32),
            pltpu.VMEM((8, 3584), F32),
            pltpu.SMEM((SEQ,), jnp.int32),
            pltpu.SemaphoreType.DMA((9,)),
            pltpu.SemaphoreType.DMA((64,)),
            pltpu.SemaphoreType.DMA((8,)),
            pltpu.SemaphoreType.DMA((1,)),
            pltpu.SemaphoreType.DMA((3,)),
            pltpu.SemaphoreType.DMA((3,)),
        ],
        compiler_params=pltpu.CompilerParams(
            collective_id=0, has_side_effects=True, vmem_limit_bytes=40 * 1024 * 1024
        ),
        name="move",
    )(*far)
    qkv_tp, out_tp, decoded = pl.pallas_call(
        write_kernel,
        out_shape=(pltpu.HBM((QC, 3584), BF16), pltpu.HBM((OC, 3584), BF16), pltpu.HBM((SEQ, OC), BF16)),
        in_specs=[vmem, vmem],
        out_specs=(hbm, hbm, hbm),
        scratch_shapes=[
            pltpu.VMEM((QC, 3584), BF16),
            pltpu.VMEM((OC, 3584), BF16),
            pltpu.SemaphoreType.DMA((10,)),
        ],
        compiler_params=pltpu.CompilerParams(vmem_limit_bytes=24 * 1024 * 1024),
        name="write",
    )(land.reshape(TILES, 3584, 128), dec)
    return decoded, qkv_tp.T, out_tp.T


def solution(mesh):
    in_specs = (
        P("rep", None),
        P("rep"),
        P(None, "tp"),
        P(None, "tp"),
        P("rep", "tp", None),
        P("rep", "tp", None),
        P(("rep", "tp"), None),
        P(("rep", "tp"), None),
    )
    out_specs = (P("rep", "tp"), P(None, "tp"), P(None, "tp"))
    return jax.shard_map(per_device, mesh=mesh, in_specs=in_specs, out_specs=out_specs, check_vma=False)
```

```python
import jax
import jax.numpy as jnp
import numpy as np
from jax import lax
from jax.experimental import pallas as pl
from jax.experimental.pallas import tpu as pltpu
from jax.sharding import PartitionSpec as P

HQ = 28
KVH = 4
HD = 128
GROUP = HQ // KVH
ROPE_BASE = 1000000.0
ROWS = 28
QC = 576
OC = 448
TILES = 8
QUADS = ROWS // 4
SEQ = 4
CHUNK = 512
PAIRS = SEQ * KVH

ITEMS = ((0, 0), (0, 1), (1, 0), (3, 0), (1, 1), (3, 1), (2, 0), (2, 1))
ROUTE = "AACCAABA"
PASS_UP = (True, False, True, False, True, False, True, True)
ORDER = (
    ("O", 0), ("O", 1), ("D", 0), ("P", 0), ("U", 0), ("O", 2), ("O", 3), ("D*", 2), ("U*", 2), ("O", 4), ("O", 5),
    ("D*", 3), ("U*", 3), ("O", 6), ("O", 7), ("D", 1), ("P", 1), ("U", 1), ("P", 2), ("V", 0), ("u", 0), ("D", 2),
    ("P", 3), ("U", 4), ("d", 0), ("D", 3), ("U", 2), ("P", 4), ("U", 5), ("V*", 2), ("U", 3), ("D", 4), ("P", 5),
    ("V*", 3), ("D", 5), ("P", 6), ("U", 6), ("D", 6), ("P", 7), ("U", 7), ("V", 2), ("D", 7), ("V", 1), ("d", 2),
    ("V", 3), ("d", 1), ("u", 1), ("u", 2), ("d", 4), ("v", 0), ("d", 3), ("V", 4), ("V", 5), ("u", 3), ("d", 5),
    ("u", 4), ("u", 6), ("V", 6), ("u", 5), ("d", 6), ("d", 7), ("u", 7), ("v", 2), ("V", 7), ("v", 3), ("v", 4),
    ("v", 1), ("v", 6), ("v", 5), ("v", 7),
)
DECODE = {
    ("O", 0): ("start", "exchange", "project",),
    ("O", 6): ("rotary", "attend0", "attend1",),
    ("U", 1): ("attend2", "attend3", "share",),
    ("V", 3): ("combine",),
    ("u", 7): ("finish",),
}
F32 = jnp.float32
BF16 = jnp.bfloat16
NT = (((1,), (1,)), ((), ()))


def move_kernel(
    lengths, hidden, freq, old_qkv, old_out, keys, values, new_qkv, new_out,
    land, decoded,
    packed, early, nq, no, hid, frq, wq, wo, kb, vb,
    jown, jall, jfull, qf, ownb, part, parts, att, attf, amat,
    lens, load_sem, recv_sem, early_sem, twin_sem, send_sem, small_recv, small_send,
):
    rep = lax.axis_index("rep")
    tp = lax.axis_index("tp")
    core = rep % 2
    x_lo = (rep // 2) % 2
    z = rep // 4
    y = tp // 2
    x_hi = tp % 2
    z_up = (z + 1) % 4
    z_dn = (z + 3) % 4
    z_op = (z + 2) % 4
    x_ot = 1 - x_lo

    def rep_of(zz, xx, cc):
        return (zz * 2 + xx) * 2 + cc

    loads = []
    for n, (src, dst) in enumerate(
        ((new_qkv, nq), (new_out, no), (hidden, hid), (freq, frq), (old_qkv, wq), (keys, kb), (values, vb), (old_out, wo), (lengths, lens))
    ):
        c = pltpu.make_async_copy(src, dst, load_sem.at[n])
        if n < 2:
            c.start()
        loads.append(c)

    barrier = pltpu.get_barrier_semaphore()
    friends = []
    for dy in range(4):
        for f in range(2):
            t = ((y + dy) % 4) * 2 + (x_hi + f) % 2
            if (dy, f) != (0, 0):
                friends.append((rep, t))
            if f == 1:
                friends.append((rep_of(z, x_ot, core), t))
    friends.append((rep_of(z, x_ot, core), tp))
    friends.append((rep_of(z_up, x_lo, core), tp))
    friends.append((rep_of(z_dn, x_lo, core), tp))
    friends.append((rep_of(z, x_lo, 1 - core), tp))
    for r, t in friends:
        pl.semaphore_signal(barrier, inc=1, device_id={"rep": r, "tp": t}, device_id_type=pl.DeviceIdType.MESH)

    loads[0].wait()
    loads[1].wait()
    for c in loads[2:]:
        c.start()
    for t in range(8):
        a = nq[:, QC * t : QC * (t + 1)]
        b = no[:, OC * t : OC * (t + 1)]
        for k in range(TILES):
            if k < 4:
                v = a[:, 128 * k : 128 * (k + 1)]
            elif k == 4:
                v = jnp.concatenate([a[:, 512:576], b[:, 384:448]], axis=1)
            else:
                v = b[:, 128 * (k - 5) : 128 * (k - 4)]
            packed[t, k] = v.reshape(QUADS, 4, 128)
    mine = rep * 8 + tp
    land[:, pl.ds(QUADS * mine, QUADS)] = packed[tp]
    pl.semaphore_wait(barrier, len(friends))

    sent = []

    def slot_key(slot):
        return slot // 16 * 8 + slot % 8

    def place(slot):
        return land.at[:, pl.ds(QUADS * slot, QUADS)]

    def put(src, slot, r, t, sem=None):
        c = pltpu.make_async_remote_copy(
            src_ref=src, dst_ref=place(slot), send_sem=send_sem.at[0],
            recv_sem=recv_sem.at[slot_key(slot)] if sem is None else sem,
            device_id={"rep": r, "tp": t}, device_id_type=pl.DeviceIdType.MESH,
        )
        c.start()
        sent.append(c)

    def arrived(slot):
        pltpu.make_async_remote_copy(
            src_ref=place(slot), dst_ref=place(slot), send_sem=send_sem.at[0],
            recv_sem=recv_sem.at[slot_key(slot)],
            device_id={"rep": rep, "tp": tp}, device_id_type=pl.DeviceIdType.MESH,
        ).wait_recv()

    def slot_of(zz, xx, item):
        dy, f = item
        r = rep_of(zz, (xx + f) % 2, core)
        t = ((y + dy) % 4) * 2 + (x_hi + f) % 2
        return r * 8 + t

    def exchange():
        for dy, f in ITEMS[1:]:
            t = ((y + 4 - dy) % 4) * 2 + (x_hi + f) % 2
            put(packed.at[t], mine, rep_of(z, (x_lo + f) % 2, core), t)

    def up(slot):
        put(place(slot), slot, rep_of(z_up, x_lo, core), tp)

    def down(slot):
        put(place(slot), slot, rep_of(z_dn, x_lo, core), tp)

    def across(slot):
        put(place(slot), slot, rep_of(z, x_ot, core), tp)

    def twin(slot, j):
        put(place(slot), slot, rep_of(z, x_lo, 1 - core), tp, twin_sem.at[j])

    EARLY = [j for j in range(8) if ROUTE[j] == "C"]

    def heir(j):
        return ((y + 4 - ITEMS[j][0]) % 4) * 2 + x_hi

    def put_early(src, j, n, r):
        m = EARLY.index(j)
        c = pltpu.make_async_remote_copy(
            src_ref=src, dst_ref=early.at[m, n], send_sem=send_sem.at[1], recv_sem=early_sem.at[m, n],
            device_id={"rep": r, "tp": tp}, device_id_type=pl.DeviceIdType.MESH,
        )
        c.start()

    def start():
        for j in EARLY:
            put_early(packed.at[heir(j)], j, 0, rep_of(z_up, x_lo, core))
            put_early(packed.at[heir(j)], j, 1, rep_of(z_dn, x_lo, core))

    def handle_early(kind, j):
        n = "DUV".index(kind)
        block = early.at[EARLY.index(j), n]
        all_bytes(block, early_sem.at[EARLY.index(j), n])
        if kind == "D" and PASS_UP[j]:
            put_early(block, j, 2, rep_of(z_up, x_lo, core))
        if kind == "U" and not PASS_UP[j]:
            put_early(block, j, 2, rep_of(z_dn, x_lo, core))
        put(block, rep_of((z_dn, z_up, z_op)[n], x_lo, core) * 8 + tp, rep, heir(j))

    def handle(kind, j):
        if kind[1:]:
            handle_early(kind[0], j)
            return
        first, fwd_up, along = ROUTE[j] == "A", PASS_UP[j], ROUTE[j] != "C"
        zz = {"o": z, "p": z, "d": z_dn, "u": z_up, "v": z_op}[kind.lower()]
        xx = x_lo if kind in "ODUV" else x_ot
        b = slot_of(zz, xx, ITEMS[j])
        if (kind, j) != ("O", 0):
            arrived(b)
        if along and (kind == "O" or (kind == "P" and first)):
            up(b)
            down(b)
        if along and ((kind == "D" and fwd_up) or (kind == "d" and first and not fwd_up)):
            up(b)
        if along and ((kind == "U" and not fwd_up) or (kind == "u" and first and fwd_up)):
            down(b)
        if kind == "O" or (kind in "DUV" and not first):
            across(b)
        twin(b, j)

    small = []

    def to_peers(phase, src_of, dst_of):
        for n in range(1, 8):
            t = (tp + n) % 8
            c = pltpu.make_async_remote_copy(
                src_ref=src_of(t), dst_ref=dst_of(), send_sem=small_send.at[phase],
                recv_sem=small_recv.at[phase],
                device_id={"rep": rep, "tp": t}, device_id_type=pl.DeviceIdType.MESH,
            )
            c.start()
            small.append(c)

    def all_bytes(ref, sem):
        pltpu.make_async_copy(ref, ref, sem).wait()

    seven = (jall.at[pl.ds(0, 7)], parts.at[pl.ds(0, 7)], att.at[pl.ds(0, 7 * 16)])

    def project():
        loads[2].wait()
        loads[4].wait()
        res = lax.dot_general(hid[...], wq[...], NT, preferred_element_type=F32).astype(BF16)
        jown[:, 0:QC] = res
        jall[tp, :, 0:QC] = res
        to_peers(0, lambda t: jown, lambda: jall.at[tp])

    def rotary():
        all_bytes(seven[0], small_recv.at[0])
        loads[3].wait()
        loads[8].wait()
        row = lax.broadcasted_iota(jnp.int32, (8, HD), 0)
        lane = lax.broadcasted_iota(jnp.int32, (8, HD), 1)
        pos = jnp.zeros((8, HD), F32)
        for s in range(SEQ):
            pos = jnp.where(row == s, lens[s].astype(F32), pos)
        angles = pos * jnp.broadcast_to(frq[0:1, :], (8, HD))
        cos2 = jnp.cos(angles)[0:SEQ]
        sin2 = jnp.where(lane < HD // 2, -jnp.sin(angles), jnp.sin(angles))[0:SEQ]
        for t in range(8):
            jfull[0:SEQ, QC * t : QC * (t + 1)] = jall[t, :, 0:QC].astype(F32)
        for h in range(HQ + KVH):
            x = jfull[0:SEQ, HD * h : HD * (h + 1)]
            r = x * cos2 + pltpu.roll(x, HD // 2, 1) * sin2
            qf[8 * h : 8 * h + SEQ, :] = r.astype(BF16).astype(F32)
        inv_root = 1.0 / jnp.sqrt(F32(HD))
        for s in range(SEQ):
            for k in range(KVH):
                q = qf[pl.ds(8 * GROUP * k + s, 8, stride=8), :]
                key = qf[8 * (HQ + k) + s : 8 * (HQ + k) + s + 1, :]
                own = jnp.sum(q * key, axis=1, keepdims=True) * inv_root
                ownb[s * KVH + k, 0:8, :] = jnp.broadcast_to(own, (8, HD))
                c0 = HQ * HD + KVH * HD + HD * k
                ownb[s * KVH + k, 8:16, :] = jnp.broadcast_to(jfull[s : s + 1, c0 : c0 + HD], (8, HD))

    def attend(s):
        if s == 0:
            loads[5].wait()
            loads[6].wait()
        inv_root = 1.0 / jnp.sqrt(F32(HD))
        pos = lax.broadcasted_iota(jnp.int32, (8, CHUNK), 1) + tp * CHUNK
        live = pos < lens[s]
        row = lax.broadcasted_iota(jnp.int32, (8, HD), 0)
        lane = lax.broadcasted_iota(jnp.int32, (8, HD), 1)
        for k in range(KVH):
            q = qf[pl.ds(8 * GROUP * k + s, 8, stride=8), :].astype(BF16)
            sc = lax.dot_general(
                q, kb[s, :, HD * k : HD * (k + 1)], NT, preferred_element_type=F32
            ) * inv_root
            sc = jnp.where(live, sc, F32(-1e30))
            m = jnp.max(sc, axis=1, keepdims=True)
            p = jnp.where(live, jnp.exp(sc - m), F32(0.0)).astype(BF16)
            l = jnp.sum(p.astype(F32), axis=1, keepdims=True)
            n = jnp.dot(p, vb[s, :, HD * k : HD * (k + 1)], preferred_element_type=F32)
            stats = jnp.sum(
                jnp.where(lane == row, jnp.broadcast_to(m, (8, HD)), 0.0)
                + jnp.where(lane == row + 8, jnp.broadcast_to(l, (8, HD)), 0.0),
                axis=0,
                keepdims=True,
            )
            part[s * KVH + k] = jnp.where(row < GROUP, n, jnp.broadcast_to(stats, (8, HD)))

    def share():
        parts[tp] = part[pl.ds(2 * tp, 2)]
        to_peers(1, lambda t: part.at[pl.ds(2 * t, 2)], lambda: parts.at[tp])

    def combine():
        all_bytes(seven[1], small_recv.at[1])
        row = lax.broadcasted_iota(jnp.int32, (8, HD), 0)
        lane = lax.broadcasted_iota(jnp.int32, (8, HD), 1)
        done = []
        for n in range(2):
            own = ownb[2 * tp + n, 0:8, :]
            val = ownb[2 * tp + n, 8:16, :]
            maxima, totals = [], []
            top = own
            for t in range(8):
                stats = jnp.broadcast_to(parts[t, n, GROUP : GROUP + 1, :], (8, HD))
                m = jnp.sum(jnp.where(lane == row, stats, 0.0), axis=1, keepdims=True)
                l = jnp.sum(jnp.where(lane == row + 8, stats, 0.0), axis=1, keepdims=True)
                maxima.append(jnp.broadcast_to(m, (8, HD)))
                totals.append(jnp.broadcast_to(l, (8, HD)))
                top = jnp.maximum(top, maxima[t])
            w = jnp.exp(own - top).astype(BF16).astype(F32)
            num = w * val
            den = w
            for t in range(8):
                scale = jnp.exp(maxima[t] - top)
                num = num + parts[t, n] * scale
                den = den + totals[t] * scale
            done.append(num / den)
        att[pl.ds(pl.multiple_of(16 * tp, 16), 16), :] = jnp.concatenate(done, axis=0).astype(BF16)
        own = att.at[pl.ds(pl.multiple_of(16 * tp, 16), 16)]
        to_peers(2, lambda t: own, lambda: own)

    def finish():
        all_bytes(seven[2], small_recv.at[2])
        loads[7].wait()
        attf[...] = att[...].astype(F32)
        for k in range(KVH):
            for g in range(GROUP):
                h = GROUP * k + g
                amat[0:SEQ, HD * h : HD * (h + 1)] = attf[pl.ds(8 * k + g, SEQ, stride=8 * KVH), :]
        decoded[...] = lax.dot_general(
            amat[0:SEQ, :].astype(BF16), wo[...], NT, preferred_element_type=F32
        ).astype(BF16)

    pieces = {"start": start, "exchange": exchange, "project": project, "rotary": rotary, "share": share, "combine": combine, "finish": finish}
    for event in ORDER:
        handle(*event)
        for piece in DECODE.get(event, ()):
            if piece.startswith("attend"):
                attend(int(piece[-1]))
            else:
                pieces[piece]()
    for j in range(8):
        all_bytes(packed, twin_sem.at[j])
    all_bytes(land.at[:, pl.ds(0, QUADS * len(sent))], send_sem.at[0])
    all_bytes(early, send_sem.at[1])
    for phase in range(3):
        all_bytes(seven[phase], small_send.at[phase])


def write_kernel(land, dec, out_q, out_o, out_d, oq, oo, sems):
    copies = []

    def out(src, dst, first, n):
        c = pltpu.make_async_copy(src.at[pl.ds(first, n)], dst.at[pl.ds(first, n)], sems.at[len(copies)])
        c.start()
        copies.append(c)

    d = pltpu.make_async_copy(dec, out_d, sems.at[9])
    d.start()
    for k in range(TILES):
        v = land[k].T
        if k < 4:
            oq[128 * k : 128 * (k + 1)] = v
        elif k == 4:
            oq[512:576] = v[0:64]
            oo[384:448] = v[64:128]
        else:
            oo[128 * (k - 5) : 128 * (k - 4)] = v
        if k < 4:
            out(oq, out_q, 128 * k, 128)
        elif k == 4:
            out(oq, out_q, 512, 64)
            out(oo, out_o, 384, 64)
        else:
            out(oo, out_o, 128 * (k - 5), 128)
    for c in copies:
        c.wait()
    d.wait()


def per_device(hidden_state, lengths, old_qkv, old_out, cache_keys, cache_values, new_qkv, new_out):
    half = ROPE_BASE ** (-2.0 * np.arange(HD // 2) / HD)
    freq = jnp.asarray(np.concatenate([half, half])[None], F32)
    any_ = pl.BlockSpec(memory_space=pl.ANY)
    hbm = pl.BlockSpec(memory_space=pltpu.HBM)
    vmem = pl.BlockSpec(memory_space=pltpu.VMEM)
    far = [
        pltpu.with_memory_space_constraint(a, pltpu.HBM)
        for a in (lengths, hidden_state, freq, old_qkv.T, old_out.T, cache_keys, cache_values, new_qkv, new_out)
    ]
    land, dec = pl.pallas_call(
        move_kernel,
        out_shape=(pltpu.VMEM((TILES, 128 * QUADS, 4, 128), BF16), pltpu.VMEM((SEQ, OC), BF16)),
        in_specs=[hbm] * 9,
        out_specs=(vmem, vmem),
        scratch_shapes=[
            pltpu.VMEM((8, TILES, QUADS, 4, 128), BF16),
            pltpu.VMEM((2, 3, TILES, QUADS, 4, 128), BF16),
            pltpu.VMEM((ROWS, 4608), BF16),
            pltpu.VMEM((ROWS, 3584), BF16),
            pltpu.VMEM((SEQ, 3584), BF16),
            pltpu.VMEM((1, HD), F32),
            pltpu.VMEM((QC, 3584), BF16),
            pltpu.VMEM((OC, 3584), BF16),
            pltpu.VMEM((SEQ, CHUNK, 512), BF16),
            pltpu.VMEM((SEQ, CHUNK, 512), BF16),
            pltpu.VMEM((SEQ, 640), BF16),
            pltpu.VMEM((8, SEQ, 640), BF16),
            pltpu.VMEM((8, 4608), F32),
            pltpu.VMEM((8 * (HQ + KVH), HD), F32),
            pltpu.VMEM((PAIRS, 16, HD), F32),
            pltpu.VMEM((PAIRS, 8, HD), F32),
            pltpu.VMEM((8, 2, 8, HD), F32),
            pltpu.VMEM((PAIRS * 8, HD), BF16),
            pltpu.VMEM((PAIRS * 8, HD), F32),
            pltpu.VMEM((8, 3584), F32),
            pltpu.SMEM((SEQ,), jnp.int32),
            pltpu.SemaphoreType.DMA((9,)),
            pltpu.SemaphoreType.DMA((64,)),
            pltpu.SemaphoreType.DMA((2, 3)),
            pltpu.SemaphoreType.DMA((8,)),
            pltpu.SemaphoreType.DMA((2,)),
            pltpu.SemaphoreType.DMA((3,)),
            pltpu.SemaphoreType.DMA((3,)),
        ],
        compiler_params=pltpu.CompilerParams(
            collective_id=0, has_side_effects=True, vmem_limit_bytes=40 * 1024 * 1024
        ),
        name="move",
    )(*far)
    qkv_tp, out_tp, decoded = pl.pallas_call(
        write_kernel,
        out_shape=(pltpu.HBM((QC, 3584), BF16), pltpu.HBM((OC, 3584), BF16), pltpu.HBM((SEQ, OC), BF16)),
        in_specs=[vmem, vmem],
        out_specs=(hbm, hbm, hbm),
        scratch_shapes=[
            pltpu.VMEM((QC, 3584), BF16),
            pltpu.VMEM((OC, 3584), BF16),
            pltpu.SemaphoreType.DMA((10,)),
        ],
        compiler_params=pltpu.CompilerParams(vmem_limit_bytes=24 * 1024 * 1024),
        name="write",
    )(land.reshape(TILES, 3584, 128), dec)
    return decoded, qkv_tp.T, out_tp.T


def solution(mesh):
    in_specs = (
        P("rep", None),
        P("rep"),
        P(None, "tp"),
        P(None, "tp"),
        P("rep", "tp", None),
        P("rep", "tp", None),
        P(("rep", "tp"), None),
        P(("rep", "tp"), None),
    )
    out_specs = (P("rep", "tp"), P(None, "tp"), P(None, "tp"))
    return jax.shard_map(per_device, mesh=mesh, in_specs=in_specs, out_specs=out_specs, check_vma=False)
```

```python
import jax
import jax.numpy as jnp
import numpy as np
from jax import lax
from jax.experimental import pallas as pl
from jax.experimental.pallas import tpu as pltpu
from jax.sharding import PartitionSpec as P

HQ = 28
KVH = 4
HD = 128
GROUP = HQ // KVH
ROPE_BASE = 1000000.0
ROWS = 28
QC = 576
OC = 448
TILES = 8
QUADS = ROWS // 4
SEQ = 4
CHUNK = 512
PAIRS = SEQ * KVH

ITEMS = ((0, 0), (0, 1), (1, 0), (3, 0), (1, 1), (3, 1), (2, 0), (2, 1))
ROUTE = "AACCAABA"
PASS_UP = (True, False, True, False, True, False, True, True)
ORDER = (
    ("O", 0), ("O", 1), ("D", 0), ("P", 0), ("U", 0), ("O", 2), ("O", 3), ("D*", 2), ("U*", 2), ("O", 4), ("O", 5),
    ("D*", 3), ("U*", 3), ("O", 6), ("O", 7), ("D", 1), ("P", 1), ("U", 1), ("P", 2), ("V", 0), ("u", 0), ("D", 2),
    ("P", 3), ("U", 4), ("d", 0), ("D", 3), ("U", 2), ("P", 4), ("U", 5), ("V*", 2), ("U", 3), ("D", 4), ("P", 5),
    ("V*", 3), ("D", 5), ("P", 6), ("U", 6), ("D", 6), ("P", 7), ("U", 7), ("V", 2), ("D", 7), ("V", 1), ("d", 2),
    ("V", 3), ("d", 1), ("u", 1), ("u", 2), ("d", 4), ("v", 0), ("d", 3), ("V", 4), ("V", 5), ("u", 3), ("d", 5),
    ("u", 4), ("u", 6), ("V", 6), ("u", 5), ("d", 6), ("d", 7), ("u", 7), ("v", 2), ("V", 7), ("v", 3), ("v", 4),
    ("v", 1), ("v", 6), ("v", 5), ("v", 7),
)
DECODE = {
    ("O", 0): ("start", "exchange", "project",),
    ("O", 6): ("rotary", "attend0", "attend1",),
    ("U", 1): ("attend2", "attend3", "share",),
    ("V", 3): ("combine",),
    ("u", 7): ("finish",),
}
F32 = jnp.float32
BF16 = jnp.bfloat16
NT = (((1,), (1,)), ((), ()))


def move_kernel(
    lengths, hidden, freq, old_qkv, old_out, keys, values, new_qkv, new_out,
    land, decoded,
    packed, early, nq, no, hid, frq, wq, wo, kb, vb,
    jown, jall, jfull, qf, ownb, part, parts, att, attf, amat,
    lens, load_sem, recv_sem, early_sem, twin_sem, send_sem, small_recv, small_send,
):
    rep = lax.axis_index("rep")
    tp = lax.axis_index("tp")
    core = rep % 2
    x_lo = (rep // 2) % 2
    z = rep // 4
    y = tp // 2
    x_hi = tp % 2
    z_up = (z + 1) % 4
    z_dn = (z + 3) % 4
    z_op = (z + 2) % 4
    x_ot = 1 - x_lo

    def rep_of(zz, xx, cc):
        return (zz * 2 + xx) * 2 + cc

    loads = []
    for n, (src, dst) in enumerate(
        ((new_qkv, nq), (new_out, no), (hidden, hid), (freq, frq), (old_qkv, wq), (keys, kb), (values, vb), (old_out, wo), (lengths, lens))
    ):
        c = pltpu.make_async_copy(src, dst, load_sem.at[n])
        if n < 2:
            c.start()
        loads.append(c)

    barrier = pltpu.get_barrier_semaphore()
    friends = []
    for dy in range(4):
        for f in range(2):
            t = ((y + dy) % 4) * 2 + (x_hi + f) % 2
            if (dy, f) != (0, 0):
                friends.append((rep, t))
            if f == 1:
                friends.append((rep_of(z, x_ot, core), t))
    friends.append((rep_of(z, x_ot, core), tp))
    friends.append((rep_of(z_up, x_lo, core), tp))
    friends.append((rep_of(z_dn, x_lo, core), tp))
    friends.append((rep_of(z, x_lo, 1 - core), tp))
    for r, t in friends:
        pl.semaphore_signal(barrier, inc=1, device_id={"rep": r, "tp": t}, device_id_type=pl.DeviceIdType.MESH)

    loads[0].wait()
    loads[1].wait()
    for c in loads[2:]:
        c.start()
    for t in range(8):
        a = nq[:, QC * t : QC * (t + 1)]
        b = no[:, OC * t : OC * (t + 1)]
        for k in range(TILES):
            if k < 4:
                v = a[:, 128 * k : 128 * (k + 1)]
            elif k == 4:
                v = jnp.concatenate([a[:, 512:576], b[:, 384:448]], axis=1)
            else:
                v = b[:, 128 * (k - 5) : 128 * (k - 4)]
            packed[t, k] = v.reshape(QUADS, 4, 128)
    mine = rep * 8 + tp
    land[:, pl.ds(QUADS * mine, QUADS)] = packed[tp]
    pl.semaphore_wait(barrier, len(friends))

    sent = []

    def slot_key(slot):
        return slot // 16 * 8 + slot % 8

    def place(slot):
        return land.at[:, pl.ds(QUADS * slot, QUADS)]

    def put(src, slot, r, t, sem=None):
        c = pltpu.make_async_remote_copy(
            src_ref=src, dst_ref=place(slot), send_sem=send_sem.at[0],
            recv_sem=recv_sem.at[slot_key(slot)] if sem is None else sem,
            device_id={"rep": r, "tp": t}, device_id_type=pl.DeviceIdType.MESH,
        )
        c.start()
        sent.append(c)

    def arrived(slot):
        pltpu.make_async_remote_copy(
            src_ref=place(slot), dst_ref=place(slot), send_sem=send_sem.at[0],
            recv_sem=recv_sem.at[slot_key(slot)],
            device_id={"rep": rep, "tp": tp}, device_id_type=pl.DeviceIdType.MESH,
        ).wait_recv()

    def slot_of(zz, xx, item):
        dy, f = item
        r = rep_of(zz, (xx + f) % 2, core)
        t = ((y + dy) % 4) * 2 + (x_hi + f) % 2
        return r * 8 + t

    def exchange():
        for dy, f in ITEMS[1:]:
            t = ((y + 4 - dy) % 4) * 2 + (x_hi + f) % 2
            put(packed.at[t], mine, rep_of(z, (x_lo + f) % 2, core), t)

    def up(slot):
        put(place(slot), slot, rep_of(z_up, x_lo, core), tp)

    def down(slot):
        put(place(slot), slot, rep_of(z_dn, x_lo, core), tp)

    def across(slot):
        put(place(slot), slot, rep_of(z, x_ot, core), tp)

    def twin(slot, j):
        put(place(slot), slot, rep_of(z, x_lo, 1 - core), tp, twin_sem.at[j])

    EARLY = [j for j in range(8) if ROUTE[j] == "C"]

    def heir(j):
        return ((y + 4 - ITEMS[j][0]) % 4) * 2 + x_hi

    def put_early(src, j, n, r):
        m = EARLY.index(j)
        c = pltpu.make_async_remote_copy(
            src_ref=src, dst_ref=early.at[m, n], send_sem=send_sem.at[1], recv_sem=early_sem.at[m, n],
            device_id={"rep": r, "tp": tp}, device_id_type=pl.DeviceIdType.MESH,
        )
        c.start()

    def start():
        for j in EARLY:
            put_early(packed.at[heir(j)], j, 0, rep_of(z_up, x_lo, core))
            put_early(packed.at[heir(j)], j, 1, rep_of(z_dn, x_lo, core))

    def handle_early(kind, j):
        n = "DUV".index(kind)
        block = early.at[EARLY.index(j), n]
        all_bytes(block, early_sem.at[EARLY.index(j), n])
        if kind == "D" and PASS_UP[j]:
            put_early(block, j, 2, rep_of(z_up, x_lo, core))
        if kind == "U" and not PASS_UP[j]:
            put_early(block, j, 2, rep_of(z_dn, x_lo, core))
        put(block, rep_of((z_dn, z_up, z_op)[n], x_lo, core) * 8 + tp, rep, heir(j))

    def handle(kind, j):
        if kind[1:]:
            handle_early(kind[0], j)
            return
        first, fwd_up, along = ROUTE[j] == "A", PASS_UP[j], ROUTE[j] != "C"
        zz = {"o": z, "p": z, "d": z_dn, "u": z_up, "v": z_op}[kind.lower()]
        xx = x_lo if kind in "ODUV" else x_ot
        b = slot_of(zz, xx, ITEMS[j])
        if (kind, j) != ("O", 0):
            arrived(b)
        if along and (kind == "O" or (kind == "P" and first)):
            up(b)
            down(b)
        if along and ((kind == "D" and fwd_up) or (kind == "d" and first and not fwd_up)):
            up(b)
        if along and ((kind == "U" and not fwd_up) or (kind == "u" and first and fwd_up)):
            down(b)
        if kind == "O" or (kind in "DUV" and not first):
            across(b)
        twin(b, j)

    small = []

    def to_peers(phase, src_of, dst_of):
        for n in range(1, 8):
            t = (tp + n) % 8
            c = pltpu.make_async_remote_copy(
                src_ref=src_of(t), dst_ref=dst_of(), send_sem=small_send.at[phase],
                recv_sem=small_recv.at[phase],
                device_id={"rep": rep, "tp": t}, device_id_type=pl.DeviceIdType.MESH,
            )
            c.start()
            small.append(c)

    def all_bytes(ref, sem):
        pltpu.make_async_copy(ref, ref, sem).wait()

    seven = (jall.at[pl.ds(0, 7)], parts.at[pl.ds(0, 7)], att.at[pl.ds(0, 7 * 16)])

    def project():
        loads[2].wait()
        loads[4].wait()
        res = lax.dot_general(hid[...], wq[...], NT, preferred_element_type=F32).astype(BF16)
        jown[:, 0:QC] = res
        jall[tp, :, 0:QC] = res
        to_peers(0, lambda t: jown, lambda: jall.at[tp])

    def rotary():
        all_bytes(seven[0], small_recv.at[0])
        loads[3].wait()
        loads[8].wait()
        row = lax.broadcasted_iota(jnp.int32, (8, HD), 0)
        lane = lax.broadcasted_iota(jnp.int32, (8, HD), 1)
        pos = jnp.zeros((8, HD), F32)
        for s in range(SEQ):
            pos = jnp.where(row == s, lens[s].astype(F32), pos)
        angles = pos * jnp.broadcast_to(frq[0:1, :], (8, HD))
        cos2 = jnp.cos(angles)[0:SEQ]
        sin2 = jnp.where(lane < HD // 2, -jnp.sin(angles), jnp.sin(angles))[0:SEQ]
        for t in range(8):
            jfull[0:SEQ, QC * t : QC * (t + 1)] = jall[t, :, 0:QC].astype(F32)
        for h in range(HQ + KVH):
            x = jfull[0:SEQ, HD * h : HD * (h + 1)]
            r = x * cos2 + pltpu.roll(x, HD // 2, 1) * sin2
            qf[8 * h : 8 * h + SEQ, :] = r.astype(BF16).astype(F32)
        inv_root = 1.0 / jnp.sqrt(F32(HD))
        for s in range(SEQ):
            for k in range(KVH):
                q = qf[pl.ds(8 * GROUP * k + s, 8, stride=8), :]
                key = qf[8 * (HQ + k) + s : 8 * (HQ + k) + s + 1, :]
                own = jnp.sum(q * key, axis=1, keepdims=True) * inv_root
                ownb[s * KVH + k, 0:8, :] = jnp.broadcast_to(own, (8, HD))
                c0 = HQ * HD + KVH * HD + HD * k
                ownb[s * KVH + k, 8:16, :] = jnp.broadcast_to(jfull[s : s + 1, c0 : c0 + HD], (8, HD))

    def attend(s):
        if s == 0:
            loads[5].wait()
            loads[6].wait()
        inv_root = 1.0 / jnp.sqrt(F32(HD))
        pos = lax.broadcasted_iota(jnp.int32, (8, CHUNK), 1) + tp * CHUNK
        live = pos < lens[s]
        row = lax.broadcasted_iota(jnp.int32, (8, HD), 0)
        lane = lax.broadcasted_iota(jnp.int32, (8, HD), 1)
        for k in range(KVH):
            q = qf[pl.ds(8 * GROUP * k + s, 8, stride=8), :].astype(BF16)
            sc = lax.dot_general(
                q, kb[s, :, HD * k : HD * (k + 1)], NT, preferred_element_type=F32
            ) * inv_root
            sc = jnp.where(live, sc, F32(-1e30))
            m = jnp.max(sc, axis=1, keepdims=True)
            p = jnp.where(live, jnp.exp(sc - m), F32(0.0)).astype(BF16)
            l = jnp.sum(p.astype(F32), axis=1, keepdims=True)
            n = jnp.dot(p, vb[s, :, HD * k : HD * (k + 1)], preferred_element_type=F32)
            stats = jnp.sum(
                jnp.where(lane == row, jnp.broadcast_to(m, (8, HD)), 0.0)
                + jnp.where(lane == row + 8, jnp.broadcast_to(l, (8, HD)), 0.0),
                axis=0,
                keepdims=True,
            )
            part[s * KVH + k] = jnp.where(row < GROUP, n, jnp.broadcast_to(stats, (8, HD)))

    def share():
        parts[tp] = part[pl.ds(2 * tp, 2)]
        to_peers(1, lambda t: part.at[pl.ds(2 * t, 2)], lambda: parts.at[tp])

    def combine():
        all_bytes(seven[1], small_recv.at[1])
        row = lax.broadcasted_iota(jnp.int32, (8, HD), 0)
        lane = lax.broadcasted_iota(jnp.int32, (8, HD), 1)
        done = []
        for n in range(2):
            own = ownb[2 * tp + n, 0:8, :]
            val = ownb[2 * tp + n, 8:16, :]
            maxima, totals = [], []
            top = own
            for t in range(8):
                stats = jnp.broadcast_to(parts[t, n, GROUP : GROUP + 1, :], (8, HD))
                m = jnp.sum(jnp.where(lane == row, stats, 0.0), axis=1, keepdims=True)
                l = jnp.sum(jnp.where(lane == row + 8, stats, 0.0), axis=1, keepdims=True)
                maxima.append(jnp.broadcast_to(m, (8, HD)))
                totals.append(jnp.broadcast_to(l, (8, HD)))
                top = jnp.maximum(top, maxima[t])
            w = jnp.exp(own - top).astype(BF16).astype(F32)
            num = w * val
            den = w
            for t in range(8):
                scale = jnp.exp(maxima[t] - top)
                num = num + parts[t, n] * scale
                den = den + totals[t] * scale
            done.append(num / den)
        att[pl.ds(pl.multiple_of(16 * tp, 16), 16), :] = jnp.concatenate(done, axis=0).astype(BF16)
        own = att.at[pl.ds(pl.multiple_of(16 * tp, 16), 16)]
        to_peers(2, lambda t: own, lambda: own)

    def finish():
        all_bytes(seven[2], small_recv.at[2])
        loads[7].wait()
        attf[...] = att[...].astype(F32)
        for k in range(KVH):
            for g in range(GROUP):
                h = GROUP * k + g
                amat[0:SEQ, HD * h : HD * (h + 1)] = attf[pl.ds(8 * k + g, SEQ, stride=8 * KVH), :]
        decoded[...] = lax.dot_general(
            amat[0:SEQ, :].astype(BF16), wo[...], NT, preferred_element_type=F32
        ).astype(BF16)

    pieces = {"start": start, "exchange": exchange, "project": project, "rotary": rotary, "share": share, "combine": combine, "finish": finish}
    for event in ORDER:
        handle(*event)
        for piece in DECODE.get(event, ()):
            if piece.startswith("attend"):
                attend(int(piece[-1]))
            else:
                pieces[piece]()
    for j in range(8):
        all_bytes(packed, twin_sem.at[j])
    all_bytes(land.at[:, pl.ds(0, QUADS * len(sent))], send_sem.at[0])
    all_bytes(early, send_sem.at[1])
    for phase in range(3):
        all_bytes(seven[phase], small_send.at[phase])


def write_kernel(land, dec, out_q, out_o, out_d, oq, oo, sems):
    copies = []

    def out(src, dst, first, n):
        c = pltpu.make_async_copy(src.at[pl.ds(first, n)], dst.at[pl.ds(first, n)], sems.at[len(copies)])
        c.start()
        copies.append(c)

    d = pltpu.make_async_copy(dec, out_d, sems.at[9])
    d.start()
    for k in (0, 1, 2, 3, 5, 6, 7, 4):
        v = land[k].T
        if k < 4:
            oq[128 * k : 128 * (k + 1)] = v
        elif k == 4:
            oq[512:576] = v[0:64]
            oo[384:448] = v[64:128]
        else:
            oo[128 * (k - 5) : 128 * (k - 4)] = v
        if k < 4:
            out(oq, out_q, 128 * k, 128)
        elif k == 4:
            out(oq, out_q, 512, 64)
            out(oo, out_o, 384, 64)
        else:
            out(oo, out_o, 128 * (k - 5), 128)
    for c in copies:
        c.wait()
    d.wait()


def per_device(hidden_state, lengths, old_qkv, old_out, cache_keys, cache_values, new_qkv, new_out):
    half = ROPE_BASE ** (-2.0 * np.arange(HD // 2) / HD)
    freq = jnp.asarray(np.concatenate([half, half])[None], F32)
    any_ = pl.BlockSpec(memory_space=pl.ANY)
    hbm = pl.BlockSpec(memory_space=pltpu.HBM)
    vmem = pl.BlockSpec(memory_space=pltpu.VMEM)
    far = [
        pltpu.with_memory_space_constraint(a, pltpu.HBM)
        for a in (lengths, hidden_state, freq, old_qkv.T, old_out.T, cache_keys, cache_values, new_qkv, new_out)
    ]
    land, dec = pl.pallas_call(
        move_kernel,
        out_shape=(pltpu.VMEM((TILES, 128 * QUADS, 4, 128), BF16), pltpu.VMEM((SEQ, OC), BF16)),
        in_specs=[hbm] * 9,
        out_specs=(vmem, vmem),
        scratch_shapes=[
            pltpu.VMEM((8, TILES, QUADS, 4, 128), BF16),
            pltpu.VMEM((2, 3, TILES, QUADS, 4, 128), BF16),
            pltpu.VMEM((ROWS, 4608), BF16),
            pltpu.VMEM((ROWS, 3584), BF16),
            pltpu.VMEM((SEQ, 3584), BF16),
            pltpu.VMEM((1, HD), F32),
            pltpu.VMEM((QC, 3584), BF16),
            pltpu.VMEM((OC, 3584), BF16),
            pltpu.VMEM((SEQ, CHUNK, 512), BF16),
            pltpu.VMEM((SEQ, CHUNK, 512), BF16),
            pltpu.VMEM((SEQ, 640), BF16),
            pltpu.VMEM((8, SEQ, 640), BF16),
            pltpu.VMEM((8, 4608), F32),
            pltpu.VMEM((8 * (HQ + KVH), HD), F32),
            pltpu.VMEM((PAIRS, 16, HD), F32),
            pltpu.VMEM((PAIRS, 8, HD), F32),
            pltpu.VMEM((8, 2, 8, HD), F32),
            pltpu.VMEM((PAIRS * 8, HD), BF16),
            pltpu.VMEM((PAIRS * 8, HD), F32),
            pltpu.VMEM((8, 3584), F32),
            pltpu.SMEM((SEQ,), jnp.int32),
            pltpu.SemaphoreType.DMA((9,)),
            pltpu.SemaphoreType.DMA((64,)),
            pltpu.SemaphoreType.DMA((2, 3)),
            pltpu.SemaphoreType.DMA((8,)),
            pltpu.SemaphoreType.DMA((2,)),
            pltpu.SemaphoreType.DMA((3,)),
            pltpu.SemaphoreType.DMA((3,)),
        ],
        compiler_params=pltpu.CompilerParams(
            collective_id=0, has_side_effects=True, vmem_limit_bytes=40 * 1024 * 1024
        ),
        name="move",
    )(*far)
    qkv_tp, out_tp, decoded = pl.pallas_call(
        write_kernel,
        out_shape=(pltpu.HBM((QC, 3584), BF16), pltpu.HBM((OC, 3584), BF16), pltpu.HBM((SEQ, OC), BF16)),
        in_specs=[vmem, vmem],
        out_specs=(hbm, hbm, hbm),
        scratch_shapes=[
            pltpu.VMEM((QC, 3584), BF16),
            pltpu.VMEM((OC, 3584), BF16),
            pltpu.SemaphoreType.DMA((10,)),
        ],
        compiler_params=pltpu.CompilerParams(vmem_limit_bytes=24 * 1024 * 1024),
        name="write",
    )(land.reshape(TILES, 3584, 128), dec)
    return decoded, qkv_tp.T, out_tp.T


def solution(mesh):
    in_specs = (
        P("rep", None),
        P("rep"),
        P(None, "tp"),
        P(None, "tp"),
        P("rep", "tp", None),
        P("rep", "tp", None),
        P(("rep", "tp"), None),
        P(("rep", "tp"), None),
    )
    out_specs = (P("rep", "tp"), P(None, "tp"), P(None, "tp"))
    return jax.shard_map(per_device, mesh=mesh, in_specs=in_specs, out_specs=out_specs, check_vma=False)
```

```python
import jax
import jax.numpy as jnp
import numpy as np
from jax import lax
from jax.experimental import pallas as pl
from jax.experimental.pallas import tpu as pltpu
from jax.sharding import PartitionSpec as P

HQ = 28
KVH = 4
HD = 128
GROUP = HQ // KVH
ROPE_BASE = 1000000.0
ROWS = 28
QC = 576
OC = 448
TILES = 8
QUADS = ROWS // 4
SEQ = 4
CHUNK = 512
PAIRS = SEQ * KVH

ITEMS = ((0, 0), (0, 1), (1, 0), (3, 0), (1, 1), (3, 1), (2, 0), (2, 1))
ROUTE = "ACCAAABA"
PASS_UP = (True, True, False, False, True, False, True, True)
ORDER = (
    ("O", 0), ("O", 1), ("D", 0), ("P", 0), ("U", 0), ("O", 2), ("O", 3), ("D*", 1), ("U*", 1), ("O", 4), ("O", 5),
    ("D*", 2), ("U*", 2), ("O", 6), ("O", 7), ("P", 1), ("V", 0), ("u", 0), ("P", 2), ("D", 1), ("U", 3), ("d", 0),
    ("P", 3), ("D", 2), ("D", 3), ("U", 1), ("U", 4), ("P", 4), ("U", 2), ("U", 5), ("V*", 1), ("P", 5), ("D", 4),
    ("V*", 2), ("P", 6), ("D", 5), ("U", 6), ("P", 7), ("D", 6), ("U", 7), ("V", 1), ("D", 7), ("v", 0), ("d", 1),
    ("V", 2), ("V", 3), ("d", 3), ("u", 1), ("d", 4), ("u", 3), ("d", 2), ("d", 5), ("u", 4), ("u", 2), ("V", 4),
    ("V", 5), ("u", 6), ("d", 7), ("u", 5), ("d", 6), ("V", 6), ("u", 7), ("v", 1), ("V", 7), ("v", 4), ("v", 2),
    ("v", 3), ("v", 5), ("v", 6), ("v", 7),
)
DECODE = {
    ("O", 0): ("start", "exchange", "project",),
    ("O", 6): ("rotary", "attend0", "attend1",),
    ("P", 1): ("attend2",),
    ("u", 0): ("attend3", "share",),
    ("d", 1): ("combine",),
    ("u", 7): ("finish",),
}
F32 = jnp.float32
BF16 = jnp.bfloat16
NT = (((1,), (1,)), ((), ()))


def move_kernel(
    lengths, hidden, freq, old_qkv, old_out, keys, values, new_qkv, new_out,
    land, decoded,
    packed, early, nq, no, hid, frq, wq, wo, kb, vb,
    jown, jall, jfull, qf, ownb, part, parts, att, attf, amat,
    lens, load_sem, recv_sem, early_sem, twin_sem, send_sem, small_recv, small_send,
):
    rep = lax.axis_index("rep")
    tp = lax.axis_index("tp")
    core = rep % 2
    x_lo = (rep // 2) % 2
    z = rep // 4
    y = tp // 2
    x_hi = tp % 2
    z_up = (z + 1) % 4
    z_dn = (z + 3) % 4
    z_op = (z + 2) % 4
    x_ot = 1 - x_lo

    def rep_of(zz, xx, cc):
        return (zz * 2 + xx) * 2 + cc

    loads = []
    for n, (src, dst) in enumerate(
        ((new_qkv, nq), (new_out, no), (hidden, hid), (freq, frq), (old_qkv, wq), (keys, kb), (values, vb), (old_out, wo), (lengths, lens))
    ):
        c = pltpu.make_async_copy(src, dst, load_sem.at[n])
        if n < 2:
            c.start()
        loads.append(c)

    barrier = pltpu.get_barrier_semaphore()
    friends = []
    for dy in range(4):
        for f in range(2):
            t = ((y + dy) % 4) * 2 + (x_hi + f) % 2
            if (dy, f) != (0, 0):
                friends.append((rep, t))
            if f == 1:
                friends.append((rep_of(z, x_ot, core), t))
    friends.append((rep_of(z, x_ot, core), tp))
    friends.append((rep_of(z_up, x_lo, core), tp))
    friends.append((rep_of(z_dn, x_lo, core), tp))
    friends.append((rep_of(z, x_lo, 1 - core), tp))
    for r, t in friends:
        pl.semaphore_signal(barrier, inc=1, device_id={"rep": r, "tp": t}, device_id_type=pl.DeviceIdType.MESH)

    loads[0].wait()
    loads[1].wait()
    for c in loads[2:]:
        c.start()
    for t in range(8):
        a = nq[:, QC * t : QC * (t + 1)]
        b = no[:, OC * t : OC * (t + 1)]
        for k in range(TILES):
            if k < 4:
                v = a[:, 128 * k : 128 * (k + 1)]
            elif k == 4:
                v = jnp.concatenate([a[:, 512:576], b[:, 384:448]], axis=1)
            else:
                v = b[:, 128 * (k - 5) : 128 * (k - 4)]
            packed[t, k] = v.reshape(QUADS, 4, 128)
    mine = rep * 8 + tp
    land[:, pl.ds(QUADS * mine, QUADS)] = packed[tp]
    pl.semaphore_wait(barrier, len(friends))

    sent = []

    def slot_key(slot):
        return slot // 16 * 8 + slot % 8

    def place(slot):
        return land.at[:, pl.ds(QUADS * slot, QUADS)]

    def put(src, slot, r, t, sem=None):
        c = pltpu.make_async_remote_copy(
            src_ref=src, dst_ref=place(slot), send_sem=send_sem.at[0],
            recv_sem=recv_sem.at[slot_key(slot)] if sem is None else sem,
            device_id={"rep": r, "tp": t}, device_id_type=pl.DeviceIdType.MESH,
        )
        c.start()
        sent.append(c)

    def arrived(slot):
        pltpu.make_async_remote_copy(
            src_ref=place(slot), dst_ref=place(slot), send_sem=send_sem.at[0],
            recv_sem=recv_sem.at[slot_key(slot)],
            device_id={"rep": rep, "tp": tp}, device_id_type=pl.DeviceIdType.MESH,
        ).wait_recv()

    def slot_of(zz, xx, item):
        dy, f = item
        r = rep_of(zz, (xx + f) % 2, core)
        t = ((y + dy) % 4) * 2 + (x_hi + f) % 2
        return r * 8 + t

    def exchange():
        for dy, f in ITEMS[1:]:
            t = ((y + 4 - dy) % 4) * 2 + (x_hi + f) % 2
            put(packed.at[t], mine, rep_of(z, (x_lo + f) % 2, core), t)

    def up(slot):
        put(place(slot), slot, rep_of(z_up, x_lo, core), tp)

    def down(slot):
        put(place(slot), slot, rep_of(z_dn, x_lo, core), tp)

    def across(slot):
        put(place(slot), slot, rep_of(z, x_ot, core), tp)

    def twin(slot, j):
        put(place(slot), slot, rep_of(z, x_lo, 1 - core), tp, twin_sem.at[j])

    EARLY = [j for j in range(8) if ROUTE[j] == "C"]

    def heir(j):
        dy, f = ITEMS[j]
        return rep_of(z, (x_lo + f) % 2, core), ((y + 4 - dy) % 4) * 2 + (x_hi + f) % 2

    def put_early(src, j, n, r):
        m = EARLY.index(j)
        c = pltpu.make_async_remote_copy(
            src_ref=src, dst_ref=early.at[m, n], send_sem=send_sem.at[1], recv_sem=early_sem.at[m, n],
            device_id={"rep": r, "tp": tp}, device_id_type=pl.DeviceIdType.MESH,
        )
        c.start()

    def start():
        for j in EARLY:
            put_early(packed.at[heir(j)[1]], j, 0, rep_of(z_up, x_lo, core))
            put_early(packed.at[heir(j)[1]], j, 1, rep_of(z_dn, x_lo, core))

    def handle_early(kind, j):
        n = "DUV".index(kind)
        block = early.at[EARLY.index(j), n]
        all_bytes(block, early_sem.at[EARLY.index(j), n])
        if kind == "D" and PASS_UP[j]:
            put_early(block, j, 2, rep_of(z_up, x_lo, core))
        if kind == "U" and not PASS_UP[j]:
            put_early(block, j, 2, rep_of(z_dn, x_lo, core))
        put(block, rep_of((z_dn, z_up, z_op)[n], x_lo, core) * 8 + tp, *heir(j))

    def handle(kind, j):
        if kind[1:]:
            handle_early(kind[0], j)
            return
        first, fwd_up, along = ROUTE[j] == "A", PASS_UP[j], ROUTE[j] != "C"
        zz = {"o": z, "p": z, "d": z_dn, "u": z_up, "v": z_op}[kind.lower()]
        xx = x_lo if kind in "ODUV" else x_ot
        b = slot_of(zz, xx, ITEMS[j])
        if (kind, j) != ("O", 0):
            arrived(b)
        if along and (kind == "O" or (kind == "P" and first)):
            up(b)
            down(b)
        if along and ((kind == "D" and fwd_up) or (kind == "d" and first and not fwd_up)):
            up(b)
        if along and ((kind == "U" and not fwd_up) or (kind == "u" and first and fwd_up)):
            down(b)
        if kind == "O" or (kind in "DUV" and not first):
            across(b)
        twin(b, j)

    small = []

    def to_peers(phase, src_of, dst_of):
        for n in range(1, 8):
            t = (tp + n) % 8
            c = pltpu.make_async_remote_copy(
                src_ref=src_of(t), dst_ref=dst_of(), send_sem=small_send.at[phase],
                recv_sem=small_recv.at[phase],
                device_id={"rep": rep, "tp": t}, device_id_type=pl.DeviceIdType.MESH,
            )
            c.start()
            small.append(c)

    def all_bytes(ref, sem):
        pltpu.make_async_copy(ref, ref, sem).wait()

    seven = (jall.at[pl.ds(0, 7)], parts.at[pl.ds(0, 7)], att.at[pl.ds(0, 7 * 16)])

    def project():
        loads[2].wait()
        loads[4].wait()
        res = lax.dot_general(hid[...], wq[...], NT, preferred_element_type=F32).astype(BF16)
        jown[:, 0:QC] = res
        jall[tp, :, 0:QC] = res
        to_peers(0, lambda t: jown, lambda: jall.at[tp])

    def rotary():
        all_bytes(seven[0], small_recv.at[0])
        loads[3].wait()
        loads[8].wait()
        row = lax.broadcasted_iota(jnp.int32, (8, HD), 0)
        lane = lax.broadcasted_iota(jnp.int32, (8, HD), 1)
        pos = jnp.zeros((8, HD), F32)
        for s in range(SEQ):
            pos = jnp.where(row == s, lens[s].astype(F32), pos)
        angles = pos * jnp.broadcast_to(frq[0:1, :], (8, HD))
        cos2 = jnp.cos(angles)[0:SEQ]
        sin2 = jnp.where(lane < HD // 2, -jnp.sin(angles), jnp.sin(angles))[0:SEQ]
        for t in range(8):
            jfull[0:SEQ, QC * t : QC * (t + 1)] = jall[t, :, 0:QC].astype(F32)
        for h in range(HQ + KVH):
            x = jfull[0:SEQ, HD * h : HD * (h + 1)]
            r = x * cos2 + pltpu.roll(x, HD // 2, 1) * sin2
            qf[8 * h : 8 * h + SEQ, :] = r.astype(BF16).astype(F32)
        inv_root = 1.0 / jnp.sqrt(F32(HD))
        for s in range(SEQ):
            for k in range(KVH):
                q = qf[pl.ds(8 * GROUP * k + s, 8, stride=8), :]
                key = qf[8 * (HQ + k) + s : 8 * (HQ + k) + s + 1, :]
                own = jnp.sum(q * key, axis=1, keepdims=True) * inv_root
                ownb[s * KVH + k, 0:8, :] = jnp.broadcast_to(own, (8, HD))
                c0 = HQ * HD + KVH * HD + HD * k
                ownb[s * KVH + k, 8:16, :] = jnp.broadcast_to(jfull[s : s + 1, c0 : c0 + HD], (8, HD))

    def attend(s):
        if s == 0:
            loads[5].wait()
            loads[6].wait()
        inv_root = 1.0 / jnp.sqrt(F32(HD))
        pos = lax.broadcasted_iota(jnp.int32, (8, CHUNK), 1) + tp * CHUNK
        live = pos < lens[s]
        row = lax.broadcasted_iota(jnp.int32, (8, HD), 0)
        lane = lax.broadcasted_iota(jnp.int32, (8, HD), 1)
        for k in range(KVH):
            q = qf[pl.ds(8 * GROUP * k + s, 8, stride=8), :].astype(BF16)
            sc = lax.dot_general(
                q, kb[s, :, HD * k : HD * (k + 1)], NT, preferred_element_type=F32
            ) * inv_root
            sc = jnp.where(live, sc, F32(-1e30))
            m = jnp.max(sc, axis=1, keepdims=True)
            p = jnp.where(live, jnp.exp(sc - m), F32(0.0)).astype(BF16)
            l = jnp.sum(p.astype(F32), axis=1, keepdims=True)
            n = jnp.dot(p, vb[s, :, HD * k : HD * (k + 1)], preferred_element_type=F32)
            stats = jnp.sum(
                jnp.where(lane == row, jnp.broadcast_to(m, (8, HD)), 0.0)
                + jnp.where(lane == row + 8, jnp.broadcast_to(l, (8, HD)), 0.0),
                axis=0,
                keepdims=True,
            )
            part[s * KVH + k] = jnp.where(row < GROUP, n, jnp.broadcast_to(stats, (8, HD)))

    def share():
        parts[tp] = part[pl.ds(2 * tp, 2)]
        to_peers(1, lambda t: part.at[pl.ds(2 * t, 2)], lambda: parts.at[tp])

    def combine():
        all_bytes(seven[1], small_recv.at[1])
        row = lax.broadcasted_iota(jnp.int32, (8, HD), 0)
        lane = lax.broadcasted_iota(jnp.int32, (8, HD), 1)
        done = []
        for n in range(2):
            own = ownb[2 * tp + n, 0:8, :]
            val = ownb[2 * tp + n, 8:16, :]
            maxima, totals = [], []
            top = own
            for t in range(8):
                stats = jnp.broadcast_to(parts[t, n, GROUP : GROUP + 1, :], (8, HD))
                m = jnp.sum(jnp.where(lane == row, stats, 0.0), axis=1, keepdims=True)
                l = jnp.sum(jnp.where(lane == row + 8, stats, 0.0), axis=1, keepdims=True)
                maxima.append(jnp.broadcast_to(m, (8, HD)))
                totals.append(jnp.broadcast_to(l, (8, HD)))
                top = jnp.maximum(top, maxima[t])
            w = jnp.exp(own - top).astype(BF16).astype(F32)
            num = w * val
            den = w
            for t in range(8):
                scale = jnp.exp(maxima[t] - top)
                num = num + parts[t, n] * scale
                den = den + totals[t] * scale
            done.append(num / den)
        att[pl.ds(pl.multiple_of(16 * tp, 16), 16), :] = jnp.concatenate(done, axis=0).astype(BF16)
        own = att.at[pl.ds(pl.multiple_of(16 * tp, 16), 16)]
        to_peers(2, lambda t: own, lambda: own)

    def finish():
        all_bytes(seven[2], small_recv.at[2])
        loads[7].wait()
        attf[...] = att[...].astype(F32)
        for k in range(KVH):
            for g in range(GROUP):
                h = GROUP * k + g
                amat[0:SEQ, HD * h : HD * (h + 1)] = attf[pl.ds(8 * k + g, SEQ, stride=8 * KVH), :]
        decoded[...] = lax.dot_general(
            amat[0:SEQ, :].astype(BF16), wo[...], NT, preferred_element_type=F32
        ).astype(BF16)

    pieces = {"start": start, "exchange": exchange, "project": project, "rotary": rotary, "share": share, "combine": combine, "finish": finish}
    for event in ORDER:
        handle(*event)
        for piece in DECODE.get(event, ()):
            if piece.startswith("attend"):
                attend(int(piece[-1]))
            else:
                pieces[piece]()
    for j in range(8):
        all_bytes(packed, twin_sem.at[j])
    all_bytes(land.at[:, pl.ds(0, QUADS * len(sent))], send_sem.at[0])
    all_bytes(early, send_sem.at[1])
    for phase in range(3):
        all_bytes(seven[phase], small_send.at[phase])


def write_kernel(land, dec, out_q, out_o, out_d, oq, oo, sems):
    copies = []

    def out(src, dst, first, n):
        c = pltpu.make_async_copy(src.at[pl.ds(first, n)], dst.at[pl.ds(first, n)], sems.at[len(copies)])
        c.start()
        copies.append(c)

    d = pltpu.make_async_copy(dec, out_d, sems.at[9])
    d.start()
    for k in (0, 1, 2, 3, 5, 6, 7, 4):
        v = land[k].T
        if k < 4:
            oq[128 * k : 128 * (k + 1)] = v
        elif k == 4:
            oq[512:576] = v[0:64]
            oo[384:448] = v[64:128]
        else:
            oo[128 * (k - 5) : 128 * (k - 4)] = v
        if k < 4:
            out(oq, out_q, 128 * k, 128)
        elif k == 4:
            out(oq, out_q, 512, 64)
            out(oo, out_o, 384, 64)
        else:
            out(oo, out_o, 128 * (k - 5), 128)
    for c in copies:
        c.wait()
    d.wait()


def per_device(hidden_state, lengths, old_qkv, old_out, cache_keys, cache_values, new_qkv, new_out):
    half = ROPE_BASE ** (-2.0 * np.arange(HD // 2) / HD)
    freq = jnp.asarray(np.concatenate([half, half])[None], F32)
    any_ = pl.BlockSpec(memory_space=pl.ANY)
    hbm = pl.BlockSpec(memory_space=pltpu.HBM)
    vmem = pl.BlockSpec(memory_space=pltpu.VMEM)
    far = [
        pltpu.with_memory_space_constraint(a, pltpu.HBM)
        for a in (lengths, hidden_state, freq, old_qkv.T, old_out.T, cache_keys, cache_values, new_qkv, new_out)
    ]
    land, dec = pl.pallas_call(
        move_kernel,
        out_shape=(pltpu.VMEM((TILES, 128 * QUADS, 4, 128), BF16), pltpu.VMEM((SEQ, OC), BF16)),
        in_specs=[hbm] * 9,
        out_specs=(vmem, vmem),
        scratch_shapes=[
            pltpu.VMEM((8, TILES, QUADS, 4, 128), BF16),
            pltpu.VMEM((ROUTE.count("C"), 3, TILES, QUADS, 4, 128), BF16),
            pltpu.VMEM((ROWS, 4608), BF16),
            pltpu.VMEM((ROWS, 3584), BF16),
            pltpu.VMEM((SEQ, 3584), BF16),
            pltpu.VMEM((1, HD), F32),
            pltpu.VMEM((QC, 3584), BF16),
            pltpu.VMEM((OC, 3584), BF16),
            pltpu.VMEM((SEQ, CHUNK, 512), BF16),
            pltpu.VMEM((SEQ, CHUNK, 512), BF16),
            pltpu.VMEM((SEQ, 640), BF16),
            pltpu.VMEM((8, SEQ, 640), BF16),
            pltpu.VMEM((8, 4608), F32),
            pltpu.VMEM((8 * (HQ + KVH), HD), F32),
            pltpu.VMEM((PAIRS, 16, HD), F32),
            pltpu.VMEM((PAIRS, 8, HD), F32),
            pltpu.VMEM((8, 2, 8, HD), F32),
            pltpu.VMEM((PAIRS * 8, HD), BF16),
            pltpu.VMEM((PAIRS * 8, HD), F32),
            pltpu.VMEM((8, 3584), F32),
            pltpu.SMEM((SEQ,), jnp.int32),
            pltpu.SemaphoreType.DMA((9,)),
            pltpu.SemaphoreType.DMA((64,)),
            pltpu.SemaphoreType.DMA((ROUTE.count("C"), 3)),
            pltpu.SemaphoreType.DMA((8,)),
            pltpu.SemaphoreType.DMA((2,)),
            pltpu.SemaphoreType.DMA((3,)),
            pltpu.SemaphoreType.DMA((3,)),
        ],
        compiler_params=pltpu.CompilerParams(
            collective_id=0, has_side_effects=True, vmem_limit_bytes=40 * 1024 * 1024
        ),
        name="move",
    )(*far)
    qkv_tp, out_tp, decoded = pl.pallas_call(
        write_kernel,
        out_shape=(pltpu.HBM((QC, 3584), BF16), pltpu.HBM((OC, 3584), BF16), pltpu.HBM((SEQ, OC), BF16)),
        in_specs=[vmem, vmem],
        out_specs=(hbm, hbm, hbm),
        scratch_shapes=[
            pltpu.VMEM((QC, 3584), BF16),
            pltpu.VMEM((OC, 3584), BF16),
            pltpu.SemaphoreType.DMA((10,)),
        ],
        compiler_params=pltpu.CompilerParams(vmem_limit_bytes=24 * 1024 * 1024),
        name="write",
    )(land.reshape(TILES, 3584, 128), dec)
    return decoded, qkv_tp.T, out_tp.T


def solution(mesh):
    in_specs = (
        P("rep", None),
        P("rep"),
        P(None, "tp"),
        P(None, "tp"),
        P("rep", "tp", None),
        P("rep", "tp", None),
        P(("rep", "tp"), None),
        P(("rep", "tp"), None),
    )
    out_specs = (P("rep", "tp"), P(None, "tp"), P(None, "tp"))
    return jax.shard_map(per_device, mesh=mesh, in_specs=in_specs, out_specs=out_specs, check_vma=False)
```
